256 devices in a mesh: lat: 64 (over x_lo, z, y), dp: 4 (over x_hi, core).
Axes of the slice: x: 4 (x_hi: 2, x_lo: 2; x = x_hi * 2 + x_lo), y: 4, z: 8, core: 2. Of those that a mesh axis runs over, the one named last changes fastest.
Arguments:
- state: float32 [4, 128, 256, 128], P('dp', 'lat'), may hold values from -6 to 6
- cotangent: float32 [4, 128, 256, 128], P('dp', 'lat'), may hold values from -0.18 to 0.18
- w_first: bfloat16 [128, 1024], replicated, may hold values from -0.5 to 0.5
- w_middle: bfloat16 [1024, 1024], replicated, may hold values from -0.1875 to 0.1875
- w_last: bfloat16 [1024, 128], replicated, may hold values from -0.1875 to 0.1875
Outputs:
- final_state: float32 [4, 128, 256, 128], P('dp', 'lat')
- grad_first: float32 [128, 1024], replicated
- grad_middle: float32 [1024, 1024], replicated
- grad_last: float32 [1024, 128], replicated
The draws below stay inside these ranges and needn't reach their ends.
All inputs are finite; a program needn't handle non-finite values.
Results may differ from the reference program's by a relative error of at most 0.0048.
Values sent between devices are 32-bit elements; how exact they have to be, the bound alone decides.
No kernel may reach another device: no remote copies, remote signals or barrier semaphores. Data moves between devices by JAX's collectives and lax.ppermute only.
A program may use at most 64 MiB of HBM per device.

```python
import math
import jax
import jax.numpy as jnp
from jax import lax

NLAT = 128
NLON = 256
MW = 64
FEAT = 128
HID = 1024
STEPS = 2
BATCH = 4


def shard_levels(stream_key, dims, cuts, least, top_value):
    factor_of = 1.0
    for position, blocks in cuts:
        heights = jax.random.uniform(jax.random.fold_in(jax.random.fold_in(stream_key, 6), position), (blocks,), jnp.float32, least / len(cuts), top_value / len(cuts))
        factor_of = factor_of * jnp.repeat(jnp.exp(heights), dims[position] // blocks).reshape((-1,) + (1,) * (len(dims) - 1 - position))
    return factor_of


def bell_draw(key, dims, width, most, split=(), held_as=jnp.bfloat16):
    level = shard_levels(key, dims, split, -0.22, 0.18) if split else 1.0
    values = jax.random.normal(key, dims, jnp.float32) * width * level
    return jnp.minimum(jnp.maximum(values, -most), most).astype(held_as)


def setup_inputs(seed: int = 0) -> dict:
    seeds = jax.random.split(jax.random.key(seed), 6)
    return {
        "state": bell_draw(seeds[0], (BATCH, NLAT, NLON, FEAT), 1.0, 6.0, ((0, 4), (1, 64)), jnp.float32),
        "cotangent": bell_draw(seeds[1], (BATCH, NLAT, NLON, FEAT), 0.03, 0.18, ((0, 4), (1, 64)), jnp.float32),
        "w_first": bell_draw(seeds[2], (FEAT, HID), FEAT ** -0.5, 0.5),
        "w_middle": bell_draw(seeds[3], (HID, HID), HID ** -0.5, 0.1875),
        "w_last": bell_draw(seeds[4], (HID, FEAT), HID ** -0.5, 0.1875),
    }


highest = lax.Precision.HIGHEST
tend_weight = 0.5

def grid_tables(lon_count, wave_count):
    lon_index = jnp.arange(lon_count, dtype=jnp.int32)
    wave_index = jnp.arange(wave_count, dtype=jnp.int32)
    phase_angle = (lon_index[:, None] * wave_index[None, :] % lon_count).astype(jnp.float32) * (2.0 * math.pi / lon_count)
    cosine = jnp.cos(phase_angle)
    sine_part = jnp.sin(phase_angle)
    analysis = jnp.stack([cosine, -sine_part], axis=2) / lon_count
    factor = jnp.where(wave_index == 0, 1.0, 2.0).astype(jnp.float32)
    synthesis = jnp.stack([cosine, -sine_part], axis=2) * factor[None, :, None]
    return (analysis, synthesis)

def legendre(wave_ids, lat_count, wave_count):
    lat_index = jnp.arange(lat_count).astype(jnp.float32)
    latitude = (lat_index + 0.5) * (math.pi / lat_count) - 0.5 * math.pi
    sine_lat = jnp.sin(latitude)
    cosine_lat = jnp.cos(latitude)
    quad_weight = cosine_lat * (math.pi / lat_count)
    order_m = wave_ids.astype(jnp.float32)
    counter = jnp.arange(1, wave_count).astype(jnp.float32)
    increments = 0.5 * jnp.log((2.0 * counter + 1.0) / (2.0 * counter))
    summed = lax.optimization_barrier(jnp.sum(jnp.where(counter[None, :] <= order_m[:, None], increments[None, :], 0.0), axis=1))
    diagonal = jnp.exp(0.5 * math.log(0.5) + summed[:, None] + order_m[:, None] * jnp.log(cosine_lat)[None, :])

    def advance(carry, offset):
        previous, current, ratio_prev = carry
        degree = order_m + offset
        ratio_new = jnp.sqrt((4.0 * degree * degree - 1.0) / (degree * degree - order_m * order_m))
        following = ratio_new[:, None] * (sine_lat[None, :] * current - previous / ratio_prev[:, None])
        return ((current, following, ratio_new), following)
    initial = (jnp.zeros_like(diagonal), diagonal, jnp.ones_like(order_m))
    _, remaining = lax.scan(advance, initial, jnp.arange(1, wave_count).astype(jnp.float32))
    poly_table = jnp.concatenate([diagonal[None], remaining], axis=0).transpose(1, 0, 2)
    degree = order_m[:, None] + jnp.arange(wave_count).astype(jnp.float32)[None, :]
    kept_mask = degree <= wave_count - 1
    poly_table = jnp.where(kept_mask[:, :, None], poly_table, 0.0)
    damping = jnp.where(kept_mask, 1.0 / (1.0 + degree * (degree + 1.0) / (wave_count * (wave_count - 1.0))), 0.0)
    return (poly_table, quad_weight, damping)

def spectral_whole(field, first, last, in_table, out_table, damping):
    wave_grid = jnp.einsum('bjxf,xmp->bjmpf', field, first, precision=highest)
    coeffs = jnp.einsum('mkj,bjmpf->bmkpf', in_table, wave_grid, precision=highest) * damping[None, :, :, None, None]
    back_grid = jnp.einsum('mkj,bmkpf->bjmpf', out_table, coeffs, precision=highest)
    return jnp.einsum('bjmpf,xmp->bjxf', back_grid, last, precision=highest)

def silu_slope(value):
    gate_sig = jax.nn.sigmoid(value)
    return gate_sig * (1.0 + value * (1.0 - gate_sig))

def hidden_rows(rows, w_first, w_middle):
    pre_first = jnp.dot(rows, w_first, preferred_element_type=jnp.float32)
    hidden_first = jax.nn.silu(pre_first).astype(jnp.bfloat16)
    pre_middle = jnp.dot(hidden_first, w_middle, preferred_element_type=jnp.float32)
    hidden_middle = jax.nn.silu(pre_middle).astype(jnp.bfloat16)
    return (pre_first, hidden_first, pre_middle, hidden_middle)

def forward_rows(rows, w_first, w_middle, w_last):
    _, _, _, hidden_middle = hidden_rows(rows, w_first, w_middle)
    return jnp.dot(hidden_middle, w_last, preferred_element_type=jnp.float32)

def backward_rows(rows, scaled, w_first, w_middle, w_last):
    pre_first, hidden_first, pre_middle, hidden_middle = hidden_rows(rows, w_first, w_middle)
    grad_last = jnp.dot(hidden_middle.T, scaled, preferred_element_type=jnp.float32)
    middle_back = jnp.dot(scaled, w_last.T, preferred_element_type=jnp.float32)
    middle_grad = (middle_back * silu_slope(pre_middle)).astype(jnp.bfloat16)
    grad_middle = jnp.dot(hidden_first.T, middle_grad, preferred_element_type=jnp.float32)
    first_back = jnp.dot(middle_grad, w_middle.T, preferred_element_type=jnp.float32)
    first_grad = (first_back * silu_slope(pre_first)).astype(jnp.bfloat16)
    grad_first = jnp.dot(rows.T, first_grad, preferred_element_type=jnp.float32)
    back_rows = jnp.dot(first_grad, w_first.T, preferred_element_type=jnp.float32)
    return ((grad_first, grad_middle, grad_last), back_rows)

def reference(state, cotangent, w_first, w_middle, w_last):
    batch, lat_count, lon_count, features = state.shape
    hidden_count = w_first.shape[1]
    analysis, synthesis = grid_tables(lon_count, MW)
    poly_table, quad_weight, damping = legendre(jnp.arange(MW, dtype=jnp.int32), lat_count, MW)
    weighted = poly_table * quad_weight[None, None, :]
    row_count = batch * lat_count * lon_count
    block = math.gcd(row_count, 8192)
    inputs = []
    field = state
    for step_index in range(STEPS):
        inputs.append(field)
        rows = field.reshape(row_count // block, block, features).astype(jnp.bfloat16)
        tendency = lax.map(lambda piece: forward_rows(piece, w_first, w_middle, w_last), rows)
        moved = field + tend_weight * tendency.reshape(field.shape)
        field = spectral_whole(moved, analysis, synthesis, weighted, poly_table, damping)
    final_state = field
    grad = cotangent
    totals = (jnp.zeros((features, hidden_count), jnp.float32), jnp.zeros((hidden_count, hidden_count), jnp.float32), jnp.zeros((hidden_count, features), jnp.float32))
    for step_index in reversed(range(STEPS)):
        pulled = spectral_whole(grad, synthesis, analysis, poly_table, weighted, damping)
        scaled = (tend_weight * pulled).astype(jnp.bfloat16).reshape(row_count // block, block, features)
        rows = inputs[step_index].reshape(row_count // block, block, features).astype(jnp.bfloat16)

        def accumulate(carry, pieces):
            grads, back_rows = backward_rows(pieces[0], pieces[1], w_first, w_middle, w_last)
            return ((carry[0] + grads[0], carry[1] + grads[1], carry[2] + grads[2]), back_rows)
        totals, back_rows = lax.scan(accumulate, totals, (rows, scaled))
        grad = pulled + back_rows.reshape(field.shape)
    return (final_state, totals[0], totals[1], totals[2])
```

```python
import functools
import math

import jax
import jax.numpy as jnp
from jax import lax
from jax.experimental import pallas as pl
from jax.experimental.pallas import tpu as pltpu
from jax.sharding import Mesh, PartitionSpec as P

MW = 64
STEPS = 2
highest = lax.Precision.HIGHEST
tend_weight = 0.5

FINE = (("xl", 2), ("z", 8), ("y", 4), ("xh", 2), ("c", 2))
ALL = tuple(name for name, _ in FINE)
LAT = ("xl", "z", "y")
SWAP = [(0, 1), (1, 0)]


def device_id(x, y, z, core):
    return ((((x % 2) * 8 + z) * 4 + y) * 2 + x // 2) * 2 + core


def reduce_groups():
    wide, deep = [], []
    for y in range(4):
        for pair in range(4):
            wide.append([device_id(x, y, 2 * pair + q, 0) for x in range(4) for q in range(2)])
    for x in range(4):
        for pair in range(4):
            wide.append(
                [device_id(x, y, (2 * pair + 1 + q) % 8, 1) for y in range(4) for q in range(2)]
            )
    for x in range(4):
        for parity in range(2):
            deep.append(
                [device_id(x, y, 2 * pair + parity, 0) for y in range(4) for pair in range(4)]
            )
    for y in range(4):
        for parity in range(2):
            deep.append(
                [device_id(x, y, 2 * pair + parity, 1) for x in range(4) for pair in range(4)]
            )
    return wide, deep


WIDE, DEEP = reduce_groups()


def exchange(value, groups):
    return lax.all_to_all(value, ALL, 0, 0, axis_index_groups=groups, tiled=True)


def grid_tables(lon_count, wave_count):
    lon_index = jnp.arange(lon_count, dtype=jnp.int32)
    wave_index = jnp.arange(wave_count, dtype=jnp.int32)
    phase_angle = (wave_index[:, None] * lon_index[None, :] % lon_count).astype(jnp.float32) * (
        2.0 * math.pi / lon_count
    )
    both = jnp.stack([jnp.cos(phase_angle), -jnp.sin(phase_angle)], axis=0)
    factor = jnp.where(wave_index == 0, 1.0, 2.0).astype(jnp.float32)
    return both / lon_count, both * factor[None, :, None]


def legendre_kernel(lat_count, wave_count, order_ref, forward_ref, backward_ref, table):
    bands = lat_count // 2
    place = lax.broadcasted_iota(jnp.int32, (1, lat_count), 1)
    lat_index = jnp.where(place >= bands, 2 * (place - bands) + 1, 2 * place).astype(jnp.float32)
    latitude = (lat_index + 0.5) * (math.pi / lat_count) - 0.5 * math.pi
    sine_lat = jnp.sin(latitude)
    cosine_lat = jnp.cos(latitude)
    quad_weight = cosine_lat * (math.pi / lat_count)
    order_m = jnp.full((1, lat_count), order_ref[0], jnp.int32).astype(jnp.float32)
    counter = lax.broadcasted_iota(jnp.int32, (1, lat_count), 1).astype(jnp.float32) + 1.0
    increments = 0.5 * jnp.log((2.0 * counter + 1.0) / (2.0 * counter))
    summed = jnp.sum(jnp.where(counter <= order_m, increments, 0.0), axis=1, keepdims=True)
    current = jnp.exp(0.5 * math.log(0.5) + summed + order_m * jnp.log(cosine_lat))
    previous = jnp.zeros_like(current)
    ratio_prev = jnp.ones_like(current)
    table[0:1, :] = current
    for offset in range(1, wave_count):
        degree = order_m + float(offset)
        ratio = jnp.sqrt((4.0 * degree * degree - 1.0) / (degree * degree - order_m * order_m))
        following = ratio * (sine_lat * current - previous / ratio_prev)
        previous, current, ratio_prev = current, following, ratio
        table[offset : offset + 1, :] = current
    degree = (
        lax.broadcasted_iota(jnp.int32, (wave_count, lat_count), 0) + order_ref[0]
    ).astype(jnp.float32)
    kept = degree <= wave_count - 1
    poly = jnp.where(kept, table[...], 0.0)
    damping = jnp.where(
        kept, 1.0 / (1.0 + degree * (degree + 1.0) / (wave_count * (wave_count - 1.0))), 0.0
    )
    weighted = poly * quad_weight
    forward_ref[...] = jnp.dot(
        poly.T, damping * weighted, precision=highest, preferred_element_type=jnp.float32
    )
    backward_ref[...] = jnp.dot(
        weighted.T, damping * poly, precision=highest, preferred_element_type=jnp.float32
    )


def legendre(order, lat_count, wave_count):
    square = jax.ShapeDtypeStruct((lat_count, lat_count), jnp.float32)
    return pl.pallas_call(
        functools.partial(legendre_kernel, lat_count, wave_count),
        out_shape=(square, square),
        in_specs=[pl.BlockSpec(memory_space=pltpu.SMEM)],
        out_specs=(pl.BlockSpec(memory_space=pltpu.VMEM),) * 2,
        scratch_shapes=[pltpu.VMEM((wave_count, lat_count), jnp.float32)],
        name="legendre",
    )(order)


def silu_slope(value):
    gate_sig = jax.nn.sigmoid(value)
    return gate_sig * (1.0 + value * (1.0 - gate_sig))


def hidden_rows(rows, w_first, w_middle):
    pre_first = jnp.dot(rows, w_first, preferred_element_type=jnp.float32)
    hidden_first = jax.nn.silu(pre_first).astype(jnp.bfloat16)
    pre_middle = jnp.dot(hidden_first, w_middle, preferred_element_type=jnp.float32)
    hidden_middle = jax.nn.silu(pre_middle).astype(jnp.bfloat16)
    return (pre_first, hidden_first, pre_middle, hidden_middle)


def sum_gradients(first, middle, last):
    hidden, features = last.shape
    core = lax.axis_index("c")
    half, part = hidden // 2, features // 2
    blocks = half // part
    packed = jnp.concatenate(
        [
            middle.reshape(2, half, hidden),
            first.reshape(2, part, hidden),
            last.reshape(2, blocks, part, features).transpose(0, 2, 1, 3).reshape(2, part, hidden),
        ],
        axis=1,
    )
    rows = packed.shape[1]
    keep = lax.dynamic_index_in_dim(packed, core, 0, keepdims=False)
    send = lax.dynamic_index_in_dim(packed, 1 - core, 0, keepdims=False)
    held = keep + lax.ppermute(send, "c", SWAP)
    wide, deep = len(WIDE[0]), len(DEEP[0])
    piece = rows // wide
    held = exchange(held.reshape(wide, piece, hidden), WIDE).sum(0)
    held = held.reshape(2, piece // 2, 8, hidden // 8).transpose(0, 2, 1, 3)
    held = exchange(held.reshape(deep, piece // 2, hidden // 8), DEEP).sum(0)
    held = exchange(jnp.broadcast_to(held[None], (deep,) + held.shape), DEEP)
    held = held.reshape(2, 8, piece // 2, hidden // 8).transpose(0, 2, 1, 3)
    held = held.reshape(piece, hidden)
    held = exchange(jnp.broadcast_to(held[None], (wide,) + held.shape), WIDE)
    held = held.reshape(rows, hidden)
    other = lax.ppermute(held, "c", SWAP)
    low = jnp.where(core == 0, held, other)
    high = jnp.where(core == 0, other, held)
    both = jnp.stack([low, high])
    middle = both[:, :half].reshape(hidden, hidden)
    first = both[:, half : half + part].reshape(features, hidden)
    last = both[:, half + part :].reshape(2, part, blocks, features)
    last = last.transpose(0, 2, 1, 3).reshape(hidden, features)
    return first, middle, last


def body(state, cotangent, w_first, w_middle, w_last):
    _, lat_rows, lon_count, features = state.shape
    hidden_count = w_first.shape[1]
    bands = lax.axis_size("xl") * lax.axis_size("z") * lax.axis_size("y")
    lat_count = lat_rows * bands
    row_count = lat_rows * lon_count
    analysis, synthesis = grid_tables(lon_count, MW)
    analysis = analysis.reshape(2 * MW, lon_count)
    synthesis = synthesis.reshape(2 * MW, lon_count)
    order = lax.axis_index(LAT).astype(jnp.int32).reshape(1)
    forward_op, backward_op = legendre(order, lat_count, MW)

    def to_waves(field, table):
        return jnp.einsum("qx,jxf->jqf", table, field, precision=highest)

    def to_grid(waves, table):
        return jnp.einsum("qx,jqf->jxf", table, waves, precision=highest)

    def spectral_pair(field, grad):
        waves = jnp.stack([to_waves(field, analysis), to_waves(grad, synthesis)])
        waves = waves.reshape(2, lat_rows, 2, MW, features).transpose(3, 0, 1, 2, 4)
        waves = waves.reshape(MW, 8, features)
        owned = lax.all_to_all(waves, LAT, 0, 0, tiled=True)
        owned = owned.reshape(bands, 2, lat_rows, 2, features).transpose(1, 2, 0, 3, 4)
        owned = owned.reshape(2, lat_count, 2 * features)
        back = jnp.stack(
            [
                jnp.dot(forward_op, owned[0], precision=highest),
                jnp.dot(backward_op, owned[1], precision=highest),
            ]
        )
        back = back.reshape(2, lat_rows, bands, 2, features).transpose(2, 0, 1, 3, 4)
        back = back.reshape(bands, 8, features)
        bands_back = lax.all_to_all(back, LAT, 0, 0, tiled=True)
        bands_back = bands_back.reshape(MW, 2, lat_rows, 2, features).transpose(1, 2, 3, 0, 4)
        bands_back = bands_back.reshape(2, lat_rows, 2 * MW, features)
        return to_grid(bands_back[0], synthesis), to_grid(bands_back[1], analysis)

    def advance(field):
        rows = field.reshape(row_count, features).astype(jnp.bfloat16)
        saved = hidden_rows(rows, w_first, w_middle)
        tendency = jnp.dot(saved[3], w_last, preferred_element_type=jnp.float32)
        return field + tend_weight * tendency.reshape(field.shape), (rows,) + saved

    def pull(pulled, saved, totals):
        scaled = (tend_weight * pulled).astype(jnp.bfloat16).reshape(row_count, features)
        rows, pre_first, hidden_first, pre_middle, hidden_middle = saved
        last = jnp.dot(hidden_middle.T, scaled, preferred_element_type=jnp.float32)
        middle_back = jnp.dot(scaled, w_last.T, preferred_element_type=jnp.float32)
        middle_grad = (middle_back * silu_slope(pre_middle)).astype(jnp.bfloat16)
        middle = jnp.dot(hidden_first.T, middle_grad, preferred_element_type=jnp.float32)
        first_back = jnp.dot(middle_grad, w_middle.T, preferred_element_type=jnp.float32)
        first_grad = (first_back * silu_slope(pre_first)).astype(jnp.bfloat16)
        first = jnp.dot(rows.T, first_grad, preferred_element_type=jnp.float32)
        found = (first, middle, last)
        if totals is not None:
            found = tuple(a + b for a, b in zip(totals, found))
        return first_grad, found

    moved, saved_0 = advance(state[0])
    field, pulled = spectral_pair(moved, cotangent[0])
    moved, saved_1 = advance(field)
    first_grad, totals = pull(pulled, saved_1, None)
    back_rows = jnp.dot(first_grad, w_first.T, preferred_element_type=jnp.float32)
    grad = pulled + back_rows.reshape(pulled.shape)
    final, pulled = spectral_pair(moved, grad)
    _, totals = pull(pulled, saved_0, totals)
    return (final[None],) + sum_gradients(*totals)


def solution(mesh):
    fine = Mesh(mesh.devices.reshape(tuple(size for _, size in FINE)), ALL)
    grid = P(("xh", "c"), LAT, None, None)
    return jax.shard_map(
        body,
        mesh=fine,
        in_specs=(grid, grid, P(), P(), P()),
        out_specs=(grid, P(), P(), P()),
        check_vma=False,
    )
```

```python
import functools
import math

import jax
import jax.numpy as jnp
from jax import lax
from jax.experimental import pallas as pl
from jax.experimental.pallas import tpu as pltpu
from jax.sharding import Mesh, PartitionSpec as P

MW = 64
NLON = 256
highest = lax.Precision.HIGHEST
tend_weight = 0.5

FINE = (("xl", 2), ("z", 8), ("y", 4), ("xh", 2), ("c", 2))
ALL = tuple(name for name, _ in FINE)
LAT = ("xl", "z", "y")
SWAP = [(0, 1), (1, 0)]


def device_id(x, y, z, core):
    return ((((x % 2) * 8 + z) * 4 + y) * 2 + x // 2) * 2 + core


def reduce_groups():
    wide, deep = [], []
    for y in range(4):
        for pair in range(4):
            wide.append([device_id(x, y, 2 * pair + q, 0) for x in range(4) for q in range(2)])
    for x in range(4):
        for pair in range(4):
            wide.append(
                [device_id(x, y, (2 * pair + 1 + q) % 8, 1) for y in range(4) for q in range(2)]
            )
    for x in range(4):
        for parity in range(2):
            deep.append(
                [device_id(x, y, 2 * pair + parity, 0) for y in range(4) for pair in range(4)]
            )
    for y in range(4):
        for parity in range(2):
            deep.append(
                [device_id(x, y, 2 * pair + parity, 1) for x in range(4) for pair in range(4)]
            )
    return wide, deep


WIDE, DEEP = reduce_groups()


def exchange(value, groups):
    return lax.all_to_all(value, ALL, 0, 0, axis_index_groups=groups, tiled=True)


def legendre_kernel(lat_count, wave_count, order_ref, forward_ref, backward_ref, table):
    bands = lat_count // 2
    place = lax.broadcasted_iota(jnp.int32, (1, lat_count), 1)
    lat_index = jnp.where(place >= bands, 2 * (place - bands) + 1, 2 * place).astype(jnp.float32)
    latitude = (lat_index + 0.5) * (math.pi / lat_count) - 0.5 * math.pi
    sine_lat = jnp.sin(latitude)
    cosine_lat = jnp.cos(latitude)
    quad_weight = cosine_lat * (math.pi / lat_count)
    order_m = jnp.full((1, lat_count), order_ref[0], jnp.int32).astype(jnp.float32)
    counter = lax.broadcasted_iota(jnp.int32, (1, lat_count), 1).astype(jnp.float32) + 1.0
    increments = 0.5 * jnp.log((2.0 * counter + 1.0) / (2.0 * counter))
    summed = jnp.sum(jnp.where(counter <= order_m, increments, 0.0), axis=1, keepdims=True)
    current = jnp.exp(0.5 * math.log(0.5) + summed + order_m * jnp.log(cosine_lat))
    previous = jnp.zeros_like(current)
    ratio_prev = jnp.ones_like(current)
    table[0:1, :] = current
    for offset in range(1, wave_count):
        degree = order_m + float(offset)
        ratio = jnp.sqrt((4.0 * degree * degree - 1.0) / (degree * degree - order_m * order_m))
        following = ratio * (sine_lat * current - previous / ratio_prev)
        previous, current, ratio_prev = current, following, ratio
        table[offset : offset + 1, :] = current
    degree = (
        lax.broadcasted_iota(jnp.int32, (wave_count, lat_count), 0) + order_ref[0]
    ).astype(jnp.float32)
    kept = degree <= wave_count - 1
    poly = jnp.where(kept, table[...], 0.0)
    damping = jnp.where(
        kept, 1.0 / (1.0 + degree * (degree + 1.0) / (wave_count * (wave_count - 1.0))), 0.0
    )
    scale = jnp.where(order_m > 0.0, 2.0 / NLON, 1.0 / NLON)
    weighted = poly * quad_weight
    poly = poly * scale
    forward_ref[...] = jnp.dot(
        poly.T, damping * weighted, precision=highest, preferred_element_type=jnp.float32
    )
    backward_ref[...] = jnp.dot(
        weighted.T, damping * poly, precision=highest, preferred_element_type=jnp.float32
    )


def legendre(order, lat_count, wave_count):
    square = jax.ShapeDtypeStruct((lat_count, lat_count), jnp.float32)
    return pl.pallas_call(
        functools.partial(legendre_kernel, lat_count, wave_count),
        out_shape=(square, square),
        in_specs=[pl.BlockSpec(memory_space=pltpu.SMEM)],
        out_specs=(pl.BlockSpec(memory_space=pltpu.VMEM),) * 2,
        scratch_shapes=[pltpu.VMEM((wave_count, lat_count), jnp.float32)],
        name="legendre",
    )(order)


def vmem(count):
    return [pl.BlockSpec(memory_space=pltpu.VMEM)] * count


def call(kernel, shapes, *operands, name, scalars=0, scratch=()):
    return pl.pallas_call(
        kernel,
        out_shape=tuple(jax.ShapeDtypeStruct(shape, dtype) for shape, dtype in shapes),
        in_specs=[pl.BlockSpec(memory_space=pltpu.SMEM)] * scalars
        + vmem(len(operands) - scalars),
        out_specs=tuple(vmem(len(shapes))),
        scratch_shapes=list(scratch),
        name=name,
        compiler_params=pltpu.CompilerParams(vmem_limit_bytes=60 * 1024 * 1024),
    )(*operands)


def mm(left, right):
    return jnp.dot(left, right, preferred_element_type=jnp.float32)


def mm_nt(left, right):
    return lax.dot_general(
        left, right, (((1,), (1,)), ((), ())), preferred_element_type=jnp.float32
    )


def mm_tn(left, right):
    return lax.dot_general(
        left, right, (((0,), (0,)), ((), ())), preferred_element_type=jnp.float32
    )


def mm_exact(left, right):
    return jnp.dot(left, right, precision=highest, preferred_element_type=jnp.float32)


def silu_pair(value):
    gate = jax.nn.sigmoid(value)
    return value * gate, gate * (1.0 + value * (1.0 - gate))


def wave_table(transposed):
    shape = (NLON, 2 * MW) if transposed else (2 * MW, NLON)
    lon = lax.broadcasted_iota(jnp.int32, shape, 0 if transposed else 1)
    row = lax.broadcasted_iota(jnp.int32, shape, 1 if transposed else 0)
    wave = jnp.where(row >= MW, row - MW, row)
    angle = ((lon * wave) & (NLON - 1)).astype(jnp.float32) * (2.0 * math.pi / NLON)
    return jnp.where(row >= MW, -jnp.sin(angle), jnp.cos(angle))


def store_waves(table, fields, out_ref):
    waves = mm_exact(table, jnp.concatenate(fields, axis=1))
    feat = fields[0].shape[1]
    for i in range(len(fields)):
        for p in range(2):
            out_ref[:, 2 * i + p, :] = waves[p * MW : (p + 1) * MW, i * feat : (i + 1) * feat]


def load_fields(table_t, waves_ref):
    columns = [
        jnp.concatenate([waves_ref[:, 2 * i, :], waves_ref[:, 2 * i + 1, :]], axis=0)
        for i in range(4)
    ]
    feat = columns[0].shape[1]
    grid = mm_exact(table_t, jnp.concatenate(columns, axis=1))
    return [grid[:, i * feat : (i + 1) * feat] for i in range(4)]


def physics(rows, w_first, w_middle, h1_ref, s1_ref, h2_ref, s2_ref, at):
    size = rows.shape[0]
    half = h1_ref.shape[2]
    value, slope = silu_pair(mm(rows, w_first[...]))
    hidden = value.astype(jnp.bfloat16)
    h1_ref[0, at : at + size, :] = hidden[:, :half]
    h1_ref[1, at : at + size, :] = hidden[:, half:]
    s1_ref[at : at + size, :] = slope
    value, slope = silu_pair(mm(hidden, w_middle[...]))
    h2_ref[at : at + size, :] = value.astype(jnp.bfloat16)
    s2_ref[at : at + size, :] = slope


def first_kernel(
    state, cotangent, w_first, w_middle, w_last,
    waves, table, table_t, h1, s1, h2, s2,
):
    table[...] = wave_table(False)
    table_t[...] = wave_table(True)
    moved = []
    for j in range(2):
        field = state[j]
        physics(field.astype(jnp.bfloat16), w_first, w_middle, h1, s1, h2, s2, j * NLON)
        tendency = mm(h2[j * NLON : (j + 1) * NLON, :], w_last[...])
        moved.append(field + tend_weight * tendency)
    store_waves(table[...], moved + [cotangent[0], cotangent[1]], waves)


def middle_kernel(
    waves_in, table, table_t, w_first, w_middle, w_last,
    waves, x, h1, h2, ga1, ga2, gt, s1, s2,
):
    fields = load_fields(table_t[...], waves_in)
    moved, grads = [], []
    for j in range(2):
        rows = slice(j * NLON, (j + 1) * NLON)
        field, pulled = fields[j], fields[2 + j]
        x[rows, :] = field.astype(jnp.bfloat16)
        physics(field.astype(jnp.bfloat16), w_first, w_middle, h1, s1, h2, s2, j * NLON)
        moved.append(field + tend_weight * mm(h2[rows, :], w_last[...]))
        scaled = (tend_weight * pulled).astype(jnp.bfloat16)
        gt[rows, :] = scaled
        back = (mm_nt(scaled, w_last[...]) * s2[rows, :]).astype(jnp.bfloat16)
        ga2[rows, :] = back
        back = (mm_nt(back, w_middle[...]) * s1[rows, :]).astype(jnp.bfloat16)
        ga1[rows, :] = back
        grads.append(pulled + mm_nt(back, w_first[...]))
    store_waves(table[...], moved + grads, waves)


def weights_kernel(x, h1, h2, ga1, ga2, gt, first, middle, last):
    first[...] = mm_tn(x[...], ga1[...])
    for h in range(2):
        middle[h] = mm_tn(h1[h], ga2[...])
    last[...] = mm_tn(h2[...], gt[...])


def last_kernel(
    core_ref, waves_in, table_t, state, h1, h2, s1, s2, w_middle, w_last, first, middle, last,
    final, keep, send, ga2, ga1, gt, last_sum, first_sum,
):
    fields = load_fields(table_t[...], waves_in)
    for j in range(2):
        rows = slice(j * NLON, (j + 1) * NLON)
        final[j] = fields[j]
        scaled = (tend_weight * fields[2 + j]).astype(jnp.bfloat16)
        gt[rows, :] = scaled
        back = (mm_nt(scaled, w_last[...]) * s2[rows, :]).astype(jnp.bfloat16)
        ga2[rows, :] = back
        back = (mm_nt(back, w_middle[...]) * s1[rows, :]).astype(jnp.bfloat16)
        ga1[rows, :] = back
    core = core_ref[0]
    rows = jnp.concatenate([state[0], state[1]], axis=0).astype(jnp.bfloat16)
    first_sum[...] = first[...] + mm_tn(rows, ga1[...])
    last_sum[...] = last[...] + mm_tn(h2[...], gt[...])
    half = h1.shape[2]
    part, blocks = half // 8, 8
    for out, which in ((send, 1 - core), (keep, core)):
        out[0:half, :] = middle[which] + mm_tn(h1[which], ga2[...])
        out[half : half + part, :] = first_sum[pl.ds(pl.multiple_of(which * part, part), part), :]
        for b in range(blocks):
            at = pl.multiple_of(which * half + b * part, part)
            out[half + part : half + 2 * part, b * 128 : (b + 1) * 128] = last_sum[
                pl.ds(at, part), :
            ]


def latitudes_kernel(owned, forward_op, backward_op, back):
    for i, operator in ((0, forward_op), (1, backward_op)):
        parts = [
            jnp.concatenate([owned[:, 4 * i + p, :], owned[:, 4 * i + 2 + p, :]], axis=0)
            for p in range(2)
        ]
        found = mm_exact(operator[...], jnp.concatenate(parts, axis=1))
        bands = owned.shape[0]
        feat = owned.shape[2]
        for j in range(2):
            for p in range(2):
                back[:, 4 * i + 2 * j + p, :] = found[
                    j * bands : (j + 1) * bands, p * feat : (p + 1) * feat
                ]


def sum_wide_kernel(parts, out):
    total = parts[0]
    for i in range(1, parts.shape[0]):
        total = total + parts[i]
    size = out.shape[1]
    for r in range(2):
        for b in range(8):
            out[r * 8 + b] = total[r * size : (r + 1) * size, b * 128 : (b + 1) * 128]


def sum_deep_kernel(parts, out):
    total = parts[0]
    for i in range(1, parts.shape[0]):
        total = total + parts[i]
    for i in range(out.shape[0]):
        out[i] = total


def spread_kernel(parts, out):
    size = parts.shape[1]
    for r in range(2):
        for b in range(8):
            piece = parts[r * 8 + b]
            for i in range(out.shape[0]):
                out[i, r * size : (r + 1) * size, b * 128 : (b + 1) * 128] = piece


def add_kernel(left, right, out):
    out[...] = left[...] + right[...]


def unpack_kernel(core_ref, own, other, first, middle, last):
    core = core_ref[0]
    half = middle.shape[0] // 2
    part, blocks = half // 8, 8
    for source, which in ((own, core), (other, 1 - core)):
        middle[pl.ds(pl.multiple_of(which * half, half), half), :] = source[0:half, :]
        first[pl.ds(pl.multiple_of(which * part, part), part), :] = source[half : half + part, :]
        for b in range(blocks):
            at = pl.multiple_of(which * half + b * part, part)
            last[pl.ds(at, part), :] = source[
                half + part : half + 2 * part, b * 128 : (b + 1) * 128
            ]


def body(state, cotangent, w_first, w_middle, w_last):
    _, lat_rows, lon_count, features = state.shape
    hidden = w_first.shape[1]
    rows = lat_rows * lon_count
    bands = lax.axis_size("xl") * lax.axis_size("z") * lax.axis_size("y")
    f32, bf16 = jnp.float32, jnp.bfloat16
    core = lax.axis_index("c").astype(jnp.int32).reshape(1)
    order = lax.axis_index(LAT).astype(jnp.int32).reshape(1)
    state, cotangent = state[0], cotangent[0]
    weights = (w_first, w_middle, w_last)
    waves_of = ((MW, 8, features), f32)
    halves = ((2, rows, hidden // 2), bf16)
    wide16, wide32 = ((rows, hidden), bf16), ((rows, hidden), f32)
    thin16 = ((rows, features), bf16)

    def cross(waves):
        owned = lax.all_to_all(waves, LAT, 0, 0, tiled=True)
        (back,) = call(
            latitudes_kernel, [waves_of], owned, forward_op, backward_op, name="latitudes"
        )
        return lax.all_to_all(back, LAT, 0, 0, tiled=True)

    forward_op, backward_op = legendre(order, lat_rows * bands, MW)
    waves, table, table_t, h1_0, s1_0, h2_0, s2_0 = call(
        first_kernel,
        [waves_of, ((2 * MW, NLON), f32), ((NLON, 2 * MW), f32), halves, wide32, wide16, wide32],
        state, cotangent, *weights,
        name="first",
    )
    waves = cross(waves)
    waves, x, h1, h2, ga1, ga2, gt = call(
        middle_kernel,
        [waves_of, thin16, halves, wide16, wide16, wide16, thin16],
        waves, table, table_t, *weights,
        name="middle",
        scratch=[pltpu.VMEM((rows, hidden), f32)] * 2,
    )
    waves = cross(waves)
    first, middle, last = call(
        weights_kernel,
        [((features, hidden), f32), ((2, hidden // 2, hidden), f32), ((hidden, features), f32)],
        x, h1, h2, ga1, ga2, gt,
        name="weights",
    )
    packed = ((hidden // 2 + features, hidden), f32)
    final, keep, send = call(
        last_kernel,
        [((lat_rows, lon_count, features), f32), packed, packed],
        core, waves, table_t, state, h1_0, h2_0, s1_0, s2_0, w_middle, w_last, first, middle, last,
        name="last",
        scalars=1,
        scratch=[
            pltpu.VMEM((rows, hidden), bf16),
            pltpu.VMEM((rows, hidden), bf16),
            pltpu.VMEM((rows, features), bf16),
            pltpu.VMEM((hidden, features), f32),
            pltpu.VMEM((features, hidden), f32),
        ],
    )
    (held,) = call(add_kernel, [packed], keep, lax.ppermute(send, "c", SWAP), name="add")
    wide, deep = len(WIDE[0]), len(DEEP[0])
    piece = packed[0][0] // wide
    held = exchange(held.reshape(wide, piece, hidden), WIDE)
    parts = ((deep, piece // 2, hidden // 8), f32)
    (held,) = call(sum_wide_kernel, [parts], held, name="sum_wide")
    held = exchange(held, DEEP)
    (held,) = call(sum_deep_kernel, [parts], held, name="sum_deep")
    held = exchange(held, DEEP)
    (held,) = call(spread_kernel, [((wide, piece, hidden), f32)], held, name="spread")
    held = exchange(held, WIDE).reshape(packed[0])
    first, middle, last = call(
        unpack_kernel,
        [((features, hidden), f32), ((hidden, hidden), f32), ((hidden, features), f32)],
        core, held, lax.ppermute(held, "c", SWAP),
        name="unpack",
        scalars=1,
    )
    return final[None], first, middle, last


def solution(mesh):
    fine = Mesh(mesh.devices.reshape(tuple(size for _, size in FINE)), ALL)
    grid = P(("xh", "c"), LAT, None, None)
    return jax.shard_map(
        body,
        mesh=fine,
        in_specs=(grid, grid, P(), P(), P()),
        out_specs=(grid, P(), P(), P()),
        check_vma=False,
    )
```

```python
import functools
import math

import jax
import jax.numpy as jnp
from jax import lax
from jax.experimental import pallas as pl
from jax.experimental.pallas import tpu as pltpu
from jax.sharding import Mesh, PartitionSpec as P

MW = 64
NLON = 256
highest = lax.Precision.HIGHEST
tend_weight = 0.5

FINE = (("xl", 2), ("z", 8), ("y", 4), ("xh", 2), ("c", 2))
ALL = tuple(name for name, _ in FINE)
LAT = ("xl", "z", "y")
SWAP = [(0, 1), (1, 0)]


def device_id(x, y, z, core):
    return ((((x % 2) * 8 + z) * 4 + y) * 2 + x // 2) * 2 + core


def reduce_groups():
    wide, deep = [], []
    for y in range(4):
        for pair in range(4):
            wide.append([device_id(x, y, 2 * pair + q, 0) for x in range(4) for q in range(2)])
    for x in range(4):
        for pair in range(4):
            wide.append(
                [device_id(x, y, (2 * pair + 1 + q) % 8, 1) for y in range(4) for q in range(2)]
            )
    for x in range(4):
        for parity in range(2):
            deep.append(
                [device_id(x, y, 2 * pair + parity, 0) for y in range(4) for pair in range(4)]
            )
    for y in range(4):
        for parity in range(2):
            deep.append(
                [device_id(x, y, 2 * pair + parity, 1) for x in range(4) for pair in range(4)]
            )
    return wide, deep


WIDE, DEEP = reduce_groups()


def exchange(value, groups):
    return lax.all_to_all(value, ALL, 0, 0, axis_index_groups=groups, tiled=True)


def legendre_kernel(lat_count, wave_count, order_ref, forward_ref, backward_ref, table):
    bands = lat_count // 2
    place = lax.broadcasted_iota(jnp.int32, (1, lat_count), 1)
    lat_index = jnp.where(place >= bands, 2 * (place - bands) + 1, 2 * place).astype(jnp.float32)
    latitude = (lat_index + 0.5) * (math.pi / lat_count) - 0.5 * math.pi
    sine_lat = jnp.sin(latitude)
    cosine_lat = jnp.cos(latitude)
    quad_weight = cosine_lat * (math.pi / lat_count)
    order_m = jnp.full((1, lat_count), order_ref[0], jnp.int32).astype(jnp.float32)
    counter = lax.broadcasted_iota(jnp.int32, (1, lat_count), 1).astype(jnp.float32) + 1.0
    increments = 0.5 * jnp.log((2.0 * counter + 1.0) / (2.0 * counter))
    summed = jnp.sum(jnp.where(counter <= order_m, increments, 0.0), axis=1, keepdims=True)
    current = jnp.exp(0.5 * math.log(0.5) + summed + order_m * jnp.log(cosine_lat))
    previous = jnp.zeros_like(current)
    ratio_prev = jnp.ones_like(current)
    table[0:1, :] = current
    for offset in range(1, wave_count):
        degree = order_m + float(offset)
        ratio = jnp.sqrt((4.0 * degree * degree - 1.0) / (degree * degree - order_m * order_m))
        following = ratio * (sine_lat * current - previous / ratio_prev)
        previous, current, ratio_prev = current, following, ratio
        table[offset : offset + 1, :] = current
    degree = (
        lax.broadcasted_iota(jnp.int32, (wave_count, lat_count), 0) + order_ref[0]
    ).astype(jnp.float32)
    kept = degree <= wave_count - 1
    poly = jnp.where(kept, table[...], 0.0)
    damping = jnp.where(
        kept, 1.0 / (1.0 + degree * (degree + 1.0) / (wave_count * (wave_count - 1.0))), 0.0
    )
    scale = jnp.where(order_m > 0.0, 2.0 / NLON, 1.0 / NLON)
    weighted = poly * quad_weight
    poly = poly * scale
    forward_ref[...] = jnp.dot(
        poly.T, damping * weighted, precision=highest, preferred_element_type=jnp.float32
    )
    backward_ref[...] = jnp.dot(
        weighted.T, damping * poly, precision=highest, preferred_element_type=jnp.float32
    )


def legendre(order, lat_count, wave_count):
    square = jax.ShapeDtypeStruct((lat_count, lat_count), jnp.float32)
    return pl.pallas_call(
        functools.partial(legendre_kernel, lat_count, wave_count),
        out_shape=(square, square),
        in_specs=[pl.BlockSpec(memory_space=pltpu.SMEM)],
        out_specs=(pl.BlockSpec(memory_space=pltpu.VMEM),) * 2,
        scratch_shapes=[pltpu.VMEM((wave_count, lat_count), jnp.float32)],
        name="legendre",
        compiler_params=pltpu.CompilerParams(vmem_limit_bytes=2 * 1024 * 1024),
    )(order)


def vmem(count):
    return [pl.BlockSpec(memory_space=pltpu.VMEM)] * count


def nbytes(shape, dtype):
    return math.prod(shape) * jnp.dtype(dtype).itemsize


def call(kernel, shapes, *operands, name, scalars=0, scratch=(), spare=4):
    held = [(operand.shape, operand.dtype) for operand in operands[scalars:]]
    held += list(shapes) + list(scratch)
    return pl.pallas_call(
        kernel,
        out_shape=tuple(jax.ShapeDtypeStruct(shape, dtype) for shape, dtype in shapes),
        in_specs=[pl.BlockSpec(memory_space=pltpu.SMEM)] * scalars
        + vmem(len(operands) - scalars),
        out_specs=tuple(vmem(len(shapes))),
        scratch_shapes=[pltpu.VMEM(shape, dtype) for shape, dtype in scratch],
        name=name,
        compiler_params=pltpu.CompilerParams(
            vmem_limit_bytes=sum(nbytes(*each) for each in held) + spare * 1024 * 1024
        ),
    )(*operands)


def mm(left, right):
    return jnp.dot(left, right, preferred_element_type=jnp.float32)


def mm_nt(left, right):
    return lax.dot_general(
        left, right, (((1,), (1,)), ((), ())), preferred_element_type=jnp.float32
    )


def mm_tn(left, right):
    return lax.dot_general(
        left, right, (((0,), (0,)), ((), ())), preferred_element_type=jnp.float32
    )


def mm_exact(left, right):
    return jnp.dot(left, right, precision=highest, preferred_element_type=jnp.float32)


def silu_pair(value):
    gate = jax.nn.sigmoid(value)
    return value * gate, gate * (1.0 + value * (1.0 - gate))


def wave_table(transposed):
    shape = (NLON, 2 * MW) if transposed else (2 * MW, NLON)
    lon = lax.broadcasted_iota(jnp.int32, shape, 0 if transposed else 1)
    row = lax.broadcasted_iota(jnp.int32, shape, 1 if transposed else 0)
    wave = jnp.where(row >= MW, row - MW, row)
    angle = ((lon * wave) & (NLON - 1)).astype(jnp.float32) * (2.0 * math.pi / NLON)
    return jnp.where(row >= MW, -jnp.sin(angle), jnp.cos(angle))


def store_waves(table, fields, out_ref):
    waves = mm_exact(table, jnp.concatenate(fields, axis=1))
    feat = fields[0].shape[1]
    for i in range(len(fields)):
        for p in range(2):
            out_ref[:, 2 * i + p, :] = waves[p * MW : (p + 1) * MW, i * feat : (i + 1) * feat]


def load_fields(table_t, waves_ref):
    columns = [
        jnp.concatenate([waves_ref[:, 2 * i, :], waves_ref[:, 2 * i + 1, :]], axis=0)
        for i in range(4)
    ]
    feat = columns[0].shape[1]
    grid = mm_exact(table_t, jnp.concatenate(columns, axis=1))
    return [grid[:, i * feat : (i + 1) * feat] for i in range(4)]


def physics(rows, w_first, w_middle, h1_ref, s1_ref, h2_ref, s2_ref, at):
    size = rows.shape[0]
    half = h1_ref.shape[2]
    value, slope = silu_pair(mm(rows, w_first[...]))
    hidden = value.astype(jnp.bfloat16)
    h1_ref[0, at : at + size, :] = hidden[:, :half]
    h1_ref[1, at : at + size, :] = hidden[:, half:]
    s1_ref[at : at + size, :] = slope
    value, slope = silu_pair(mm(hidden, w_middle[...]))
    h2_ref[at : at + size, :] = value.astype(jnp.bfloat16)
    s2_ref[at : at + size, :] = slope


def first_kernel(
    state, cotangent, w_first, w_middle, w_last,
    waves, table, table_t, h1, s1, h2, s2,
):
    table[...] = wave_table(False)
    table_t[...] = wave_table(True)
    moved = []
    for j in range(2):
        field = state[j]
        physics(field.astype(jnp.bfloat16), w_first, w_middle, h1, s1, h2, s2, j * NLON)
        tendency = mm(h2[j * NLON : (j + 1) * NLON, :], w_last[...])
        moved.append(field + tend_weight * tendency)
    store_waves(table[...], moved + [cotangent[0], cotangent[1]], waves)


def middle_kernel(
    waves_in, table, table_t, w_first, w_middle, w_last,
    waves, x, h1, h2, ga1, ga2, gt, s1, s2,
):
    fields = load_fields(table_t[...], waves_in)
    moved, grads = [], []
    for j in range(2):
        rows = slice(j * NLON, (j + 1) * NLON)
        field, pulled = fields[j], fields[2 + j]
        x[rows, :] = field.astype(jnp.bfloat16)
        physics(field.astype(jnp.bfloat16), w_first, w_middle, h1, s1, h2, s2, j * NLON)
        moved.append(field + tend_weight * mm(h2[rows, :], w_last[...]))
        scaled = (tend_weight * pulled).astype(jnp.bfloat16)
        gt[rows, :] = scaled
        back = (mm_nt(scaled, w_last[...]) * s2[rows, :]).astype(jnp.bfloat16)
        ga2[rows, :] = back
        back = (mm_nt(back, w_middle[...]) * s1[rows, :]).astype(jnp.bfloat16)
        ga1[rows, :] = back
        grads.append(pulled + mm_nt(back, w_first[...]))
    store_waves(table[...], moved + grads, waves)


def weights_kernel(x, h1, h2, ga1, ga2, gt, first, middle, last):
    first[...] = mm_tn(x[...], ga1[...])
    for h in range(2):
        middle[h] = mm_tn(h1[h], ga2[...])
    last[...] = mm_tn(h2[...], gt[...])


def last_kernel(
    core_ref, waves_in, table_t, h1, h2, s2, w_last, middle,
    final, send, ga2, gt,
):
    fields = load_fields(table_t[...], waves_in)
    for j in range(2):
        rows = slice(j * NLON, (j + 1) * NLON)
        final[j] = fields[j]
        scaled = (tend_weight * fields[2 + j]).astype(jnp.bfloat16)
        gt[rows, :] = scaled
        ga2[rows, :] = (mm_nt(scaled, w_last[...]) * s2[rows, :]).astype(jnp.bfloat16)
    which = 1 - core_ref[0]
    send[...] = middle[which] + mm_tn(h1[which], ga2[...])


def rest_kernel(
    core_ref, state, h1, h2, s1, ga2, gt, w_middle, first, middle, last,
    keep, keep_thin, send_thin, ga1, first_sum, last_sum,
):
    for j in range(2):
        rows = slice(j * NLON, (j + 1) * NLON)
        back = mm_nt(ga2[rows, :], w_middle[...])
        ga1[rows, :] = (back * s1[rows, :]).astype(jnp.bfloat16)
    rows = jnp.concatenate([state[0], state[1]], axis=0).astype(jnp.bfloat16)
    first_sum[...] = first[...] + mm_tn(rows, ga1[...])
    last_sum[...] = last[...] + mm_tn(h2[...], gt[...])
    core = core_ref[0]
    half = h1.shape[2]
    part, blocks = half // 8, 8
    for out, which in ((send_thin, 1 - core), (keep_thin, core)):
        out[0:part, :] = first_sum[pl.ds(pl.multiple_of(which * part, part), part), :]
        for b in range(blocks):
            at = pl.multiple_of(which * half + b * part, part)
            out[part : 2 * part, b * 128 : (b + 1) * 128] = last_sum[pl.ds(at, part), :]
    keep[...] = middle[core] + mm_tn(h1[core], ga2[...])


def latitudes_kernel(owned, forward_op, backward_op, back):
    for i, operator in ((0, forward_op), (1, backward_op)):
        parts = [
            jnp.concatenate([owned[:, 4 * i + p, :], owned[:, 4 * i + 2 + p, :]], axis=0)
            for p in range(2)
        ]
        found = mm_exact(operator[...], jnp.concatenate(parts, axis=1))
        bands = owned.shape[0]
        feat = owned.shape[2]
        for j in range(2):
            for p in range(2):
                back[:, 4 * i + 2 * j + p, :] = found[
                    j * bands : (j + 1) * bands, p * feat : (p + 1) * feat
                ]


def sum_wide_kernel(parts, out):
    total = parts[0]
    for i in range(1, parts.shape[0]):
        total = total + parts[i]
    size = out.shape[1]
    for r in range(2):
        for b in range(8):
            out[r * 8 + b] = total[r * size : (r + 1) * size, b * 128 : (b + 1) * 128]


def sum_deep_kernel(parts, out):
    total = parts[0]
    for i in range(1, parts.shape[0]):
        total = total + parts[i]
    for i in range(out.shape[0]):
        out[i] = total


def spread_kernel(parts, out):
    size = parts.shape[1]
    for r in range(2):
        for b in range(8):
            piece = parts[r * 8 + b]
            for i in range(out.shape[0]):
                out[i, r * size : (r + 1) * size, b * 128 : (b + 1) * 128] = piece


def add_kernel(left, left_thin, right, right_thin, out):
    half = left.shape[0]
    out[0:half, :] = left[...] + right[...]
    out[half:, :] = left_thin[...] + right_thin[...]


def place(core_ref, other, source, outs, sem):
    first, middle, last = outs
    which = 1 - core_ref[0] if other else core_ref[0]
    half = middle.shape[0] // 2
    part, blocks = half // 8, 8
    copies = [
        (source.at[pl.ds(0, half)], middle.at[pl.ds(pl.multiple_of(which * half, half), half)]),
        (
            source.at[pl.ds(half, part)],
            first.at[pl.ds(pl.multiple_of(which * part, part), part)],
        ),
    ]
    for b in range(blocks):
        at = pl.multiple_of(which * half + b * part, part)
        copies.append(
            (
                source.at[pl.ds(half + part, part), pl.ds(b * 128, 128)],
                last.at[pl.ds(at, part)],
            )
        )
    started = [
        pltpu.make_async_copy(start, end, sem.at[i]) for i, (start, end) in enumerate(copies)
    ]
    for copy in started:
        copy.start()
    for copy in started:
        copy.wait()


def own_kernel(core_ref, source, first, middle, last, sem):
    place(core_ref, False, source, (first, middle, last), sem)


def other_kernel(core_ref, source, _first, _middle, _last, first, middle, last, sem):
    place(core_ref, True, source, (first, middle, last), sem)


def unpack(core, own, other, hidden, features):
    outs = [
        jax.ShapeDtypeStruct(shape, jnp.float32)
        for shape in ((features, hidden), (hidden, hidden), (hidden, features))
    ]
    smem = pl.BlockSpec(memory_space=pltpu.SMEM)
    hbm = pl.BlockSpec(memory_space=pltpu.HBM)
    settings = dict(
        out_shape=tuple(outs),
        out_specs=(hbm,) * 3,
        scratch_shapes=[pltpu.SemaphoreType.DMA((10,))],
        compiler_params=pltpu.CompilerParams(vmem_limit_bytes=4 * 1024 * 1024),
    )
    grads = pl.pallas_call(own_kernel, in_specs=[smem] + vmem(1), name="own", **settings)(core, own)
    return pl.pallas_call(
        other_kernel,
        in_specs=[smem] + vmem(1) + [hbm] * 3,
        input_output_aliases={2: 0, 3: 1, 4: 2},
        name="other",
        **settings,
    )(core, other, *grads)


def body(state, cotangent, w_first, w_middle, w_last):
    _, lat_rows, lon_count, features = state.shape
    hidden = w_first.shape[1]
    rows = lat_rows * lon_count
    bands = lax.axis_size("xl") * lax.axis_size("z") * lax.axis_size("y")
    f32, bf16 = jnp.float32, jnp.bfloat16
    core = lax.axis_index("c").astype(jnp.int32).reshape(1)
    order = lax.axis_index(LAT).astype(jnp.int32).reshape(1)
    state, cotangent = state[0], cotangent[0]
    weights = (w_first, w_middle, w_last)
    waves_of = ((MW, 8, features), f32)
    halves = ((2, rows, hidden // 2), bf16)
    wide16, wide32 = ((rows, hidden), bf16), ((rows, hidden), f32)
    thin16 = ((rows, features), bf16)

    def cross(waves):
        owned = lax.all_to_all(waves, LAT, 0, 0, tiled=True)
        (back,) = call(
            latitudes_kernel, [waves_of], owned, forward_op, backward_op, name="latitudes"
        )
        return lax.all_to_all(back, LAT, 0, 0, tiled=True)

    forward_op, backward_op = legendre(order, lat_rows * bands, MW)
    waves, table, table_t, h1_0, s1_0, h2_0, s2_0 = call(
        first_kernel,
        [waves_of, ((2 * MW, NLON), f32), ((NLON, 2 * MW), f32), halves, wide32, wide16, wide32],
        state, cotangent, *weights,
        name="first",
    )
    waves = cross(waves)
    waves, x, h1, h2, ga1, ga2, gt = call(
        middle_kernel,
        [waves_of, thin16, halves, wide16, wide16, wide16, thin16],
        waves, table, table_t, *weights,
        name="middle",
        scratch=[wide32] * 2,
    )
    waves = cross(waves)
    first, middle, last = call(
        weights_kernel,
        [((features, hidden), f32), ((2, hidden // 2, hidden), f32), ((hidden, features), f32)],
        x, h1, h2, ga1, ga2, gt,
        name="weights",
    )
    packed = ((hidden // 2 + features, hidden), f32)
    half32, thin32 = ((hidden // 2, hidden), f32), ((features, hidden), f32)
    final, send, ga2, gt = call(
        last_kernel,
        [((lat_rows, lon_count, features), f32), half32, wide16, thin16],
        core, waves, table_t, h1_0, h2_0, s2_0, w_last, middle,
        name="last",
        scalars=1,
    )
    received = lax.ppermute(send, "c", SWAP)
    keep, keep_thin, send_thin = call(
        rest_kernel,
        [half32, thin32, thin32],
        core, state, h1_0, h2_0, s1_0, ga2, gt, w_middle, first, middle, last,
        name="rest",
        scalars=1,
        scratch=[wide16, thin32, ((hidden, features), f32)],
    )
    (held,) = call(
        add_kernel, [packed], keep, keep_thin, received, lax.ppermute(send_thin, "c", SWAP),
        name="add",
    )
    wide, deep = len(WIDE[0]), len(DEEP[0])
    piece = packed[0][0] // wide
    held = exchange(held.reshape(wide, piece, hidden), WIDE)
    parts = ((deep, piece // 2, hidden // 8), f32)
    (held,) = call(sum_wide_kernel, [parts], held, name="sum_wide")
    held = exchange(held, DEEP)
    (held,) = call(sum_deep_kernel, [parts], held, name="sum_deep")
    held = exchange(held, DEEP)
    (held,) = call(spread_kernel, [((wide, piece, hidden), f32)], held, name="spread")
    held = exchange(held, WIDE).reshape(packed[0])
    other = lax.ppermute(held, "c", SWAP)
    first, middle, last = unpack(core, held, other, hidden, features)
    return final[None], first, middle, last


def solution(mesh):
    fine = Mesh(mesh.devices.reshape(tuple(size for _, size in FINE)), ALL)
    grid = P(("xh", "c"), LAT, None, None)
    return jax.shard_map(
        body,
        mesh=fine,
        in_specs=(grid, grid, P(), P(), P()),
        out_specs=(grid, P(), P(), P()),
        check_vma=False,
    )
```

```python
import functools
import math

import jax
import jax.numpy as jnp
from jax import lax
from jax.experimental import pallas as pl
from jax.experimental.pallas import tpu as pltpu
from jax.sharding import Mesh, PartitionSpec as P

MW = 64
NLON = 256
highest = lax.Precision.HIGHEST
tend_weight = 0.5

FINE = (("xl", 2), ("z", 8), ("y", 4), ("xh", 2), ("c", 2))
ALL = tuple(name for name, _ in FINE)
LAT = ("xl", "z", "y")
SWAP = [(0, 1), (1, 0)]


def device_id(x, y, z, core):
    return ((((x % 2) * 8 + z) * 4 + y) * 2 + x // 2) * 2 + core


def reduce_groups():
    wide, deep = [], []
    for y in range(4):
        for pair in range(4):
            wide.append([device_id(x, y, 2 * pair + q, 0) for x in range(4) for q in range(2)])
    for x in range(4):
        for pair in range(4):
            wide.append(
                [device_id(x, y, (2 * pair + 1 + q) % 8, 1) for y in range(4) for q in range(2)]
            )
    for x in range(4):
        for parity in range(2):
            deep.append(
                [device_id(x, y, 2 * pair + parity, 0) for y in range(4) for pair in range(4)]
            )
    for y in range(4):
        for parity in range(2):
            deep.append(
                [device_id(x, y, 2 * pair + parity, 1) for x in range(4) for pair in range(4)]
            )
    return wide, deep


WIDE, DEEP = reduce_groups()


def exchange(value, groups):
    return lax.all_to_all(value, ALL, 0, 0, axis_index_groups=groups, tiled=True)


def legendre(lat_count, wave_count, ids, forward_ref, backward_ref, table):
    bands = lat_count // 2
    place = lax.broadcasted_iota(jnp.int32, (1, lat_count), 1)
    lat_index = jnp.where(place >= bands, 2 * (place - bands) + 1, 2 * place).astype(jnp.float32)
    latitude = (lat_index + 0.5) * (math.pi / lat_count) - 0.5 * math.pi
    sine_lat = jnp.sin(latitude)
    cosine_lat = jnp.cos(latitude)
    quad_weight = cosine_lat * (math.pi / lat_count)
    order_m = jnp.full((1, lat_count), ids[0], jnp.int32).astype(jnp.float32)
    counter = lax.broadcasted_iota(jnp.int32, (1, lat_count), 1).astype(jnp.float32) + 1.0
    increments = 0.5 * jnp.log((2.0 * counter + 1.0) / (2.0 * counter))
    summed = jnp.sum(jnp.where(counter <= order_m, increments, 0.0), axis=1, keepdims=True)
    current = jnp.exp(0.5 * math.log(0.5) + summed + order_m * jnp.log(cosine_lat))
    previous = jnp.zeros_like(current)
    ratio_prev = jnp.ones_like(current)
    table[0:1, :] = current
    for offset in range(1, wave_count):
        degree = order_m + float(offset)
        ratio = jnp.sqrt((4.0 * degree * degree - 1.0) / (degree * degree - order_m * order_m))
        following = ratio * (sine_lat * current - previous / ratio_prev)
        previous, current, ratio_prev = current, following, ratio
        table[offset : offset + 1, :] = current
    degree = (
        lax.broadcasted_iota(jnp.int32, (wave_count, lat_count), 0) + ids[0]
    ).astype(jnp.float32)
    kept = degree <= wave_count - 1
    poly = jnp.where(kept, table[...], 0.0)
    damping = jnp.where(
        kept, 1.0 / (1.0 + degree * (degree + 1.0) / (wave_count * (wave_count - 1.0))), 0.0
    )
    scale = jnp.where(order_m > 0.0, 2.0 / NLON, 1.0 / NLON)
    weighted = poly * quad_weight
    poly = poly * scale
    forward_ref[...] = jnp.dot(
        poly.T, damping * weighted, precision=highest, preferred_element_type=jnp.float32
    )
    backward_ref[...] = jnp.dot(
        weighted.T, damping * poly, precision=highest, preferred_element_type=jnp.float32
    )


def vmem(count):
    return [pl.BlockSpec(memory_space=pltpu.VMEM)] * count


def nbytes(shape, dtype):
    return math.prod(shape) * jnp.dtype(dtype).itemsize


def call(kernel, shapes, *operands, name, scalars=0, scratch=(), spare=4):
    held = [(operand.shape, operand.dtype) for operand in operands[scalars:]]
    held += list(shapes) + list(scratch)
    return pl.pallas_call(
        kernel,
        out_shape=tuple(jax.ShapeDtypeStruct(shape, dtype) for shape, dtype in shapes),
        in_specs=[pl.BlockSpec(memory_space=pltpu.SMEM)] * scalars
        + vmem(len(operands) - scalars),
        out_specs=tuple(vmem(len(shapes))),
        scratch_shapes=[pltpu.VMEM(shape, dtype) for shape, dtype in scratch],
        name=name,
        compiler_params=pltpu.CompilerParams(
            vmem_limit_bytes=sum(nbytes(*each) for each in held) + spare * 1024 * 1024
        ),
    )(*operands)


def mm(left, right):
    return jnp.dot(left, right, preferred_element_type=jnp.float32)


def mm_nt(left, right):
    return lax.dot_general(
        left, right, (((1,), (1,)), ((), ())), preferred_element_type=jnp.float32
    )


def mm_tn(left, right):
    return lax.dot_general(
        left, right, (((0,), (0,)), ((), ())), preferred_element_type=jnp.float32
    )


def mm_exact(left, right):
    return jnp.dot(left, right, precision=highest, preferred_element_type=jnp.float32)


def silu_pair(value):
    gate = jax.nn.sigmoid(value)
    return value * gate, gate * (1.0 + value * (1.0 - gate))


def wave_table(transposed):
    shape = (NLON, 2 * MW) if transposed else (2 * MW, NLON)
    lon = lax.broadcasted_iota(jnp.int32, shape, 0 if transposed else 1)
    row = lax.broadcasted_iota(jnp.int32, shape, 1 if transposed else 0)
    wave = jnp.where(row >= MW, row - MW, row)
    angle = ((lon * wave) & (NLON - 1)).astype(jnp.float32) * (2.0 * math.pi / NLON)
    return jnp.where(row >= MW, -jnp.sin(angle), jnp.cos(angle))


def store_waves(table, fields, out_ref):
    waves = mm_exact(table, jnp.concatenate(fields, axis=1))
    feat = fields[0].shape[1]
    for i in range(len(fields)):
        for p in range(2):
            out_ref[:, 2 * i + p, :] = waves[p * MW : (p + 1) * MW, i * feat : (i + 1) * feat]


def load_fields(table_t, waves_ref):
    columns = [
        jnp.concatenate([waves_ref[:, 2 * i, :], waves_ref[:, 2 * i + 1, :]], axis=0)
        for i in range(4)
    ]
    feat = columns[0].shape[1]
    grid = mm_exact(table_t, jnp.concatenate(columns, axis=1))
    return [grid[:, i * feat : (i + 1) * feat] for i in range(4)]


def physics(rows, w_first, w_middle, h1_ref, s1_ref, h2_ref, s2_ref, at):
    size = rows.shape[0]
    half = h1_ref.shape[2]
    value, slope = silu_pair(mm(rows, w_first[...]))
    hidden = value.astype(jnp.bfloat16)
    h1_ref[0, at : at + size, :] = hidden[:, :half]
    h1_ref[1, at : at + size, :] = hidden[:, half:]
    s1_ref[at : at + size, :] = slope
    value, slope = silu_pair(mm(hidden, w_middle[...]))
    h2_ref[at : at + size, :] = value.astype(jnp.bfloat16)
    s2_ref[at : at + size, :] = slope


def tables_kernel(ids, table, table_t, forward_op, backward_op, poly):
    table[...] = wave_table(False)
    table_t[...] = wave_table(True)
    legendre(forward_op.shape[0], MW, ids, forward_op, backward_op, poly)


def first_kernel(
    state, cotangent, table, w_first, w_middle, w_last,
    waves, x, h1, s1, h2, s2,
):
    moved = []
    for j in range(2):
        rows = slice(j * NLON, (j + 1) * NLON)
        field = state[j]
        x[rows, :] = field.astype(jnp.bfloat16)
        physics(field.astype(jnp.bfloat16), w_first, w_middle, h1, s1, h2, s2, j * NLON)
        moved.append(field + tend_weight * mm(h2[rows, :], w_last[...]))
    store_waves(table[...], moved + [cotangent[0], cotangent[1]], waves)


def middle_kernel(
    waves_in, table, table_t, w_first, w_middle, w_last,
    waves, x, h1, h2, ga1, ga2, gt, s1, s2,
):
    fields = load_fields(table_t[...], waves_in)
    moved, grads = [], []
    for j in range(2):
        rows = slice(j * NLON, (j + 1) * NLON)
        field, pulled = fields[j], fields[2 + j]
        x[rows, :] = field.astype(jnp.bfloat16)
        physics(field.astype(jnp.bfloat16), w_first, w_middle, h1, s1, h2, s2, j * NLON)
        moved.append(field + tend_weight * mm(h2[rows, :], w_last[...]))
        scaled = (tend_weight * pulled).astype(jnp.bfloat16)
        gt[rows, :] = scaled
        back = (mm_nt(scaled, w_last[...]) * s2[rows, :]).astype(jnp.bfloat16)
        ga2[rows, :] = back
        back = (mm_nt(back, w_middle[...]) * s1[rows, :]).astype(jnp.bfloat16)
        ga1[rows, :] = back
        grads.append(pulled + mm_nt(back, w_first[...]))
    store_waves(table[...], moved + grads, waves)


def last_kernel(
    ids, waves_in, table_t, h1_0, s2, h1_1, ga2_1, w_last,
    final, send, ga2, gt,
):
    fields = load_fields(table_t[...], waves_in)
    for j in range(2):
        rows = slice(j * NLON, (j + 1) * NLON)
        final[j] = fields[j]
        scaled = (tend_weight * fields[2 + j]).astype(jnp.bfloat16)
        gt[rows, :] = scaled
        ga2[rows, :] = (mm_nt(scaled, w_last[...]) * s2[rows, :]).astype(jnp.bfloat16)
    which = 1 - ids[1]
    send[...] = mm_tn(h1_0[which], ga2[...]) + mm_tn(h1_1[which], ga2_1[...])


def thin_kernel(
    ids, x_0, h2_0, s1, ga2, gt_0, w_middle, x_1, h2_1, ga1_1, gt_1,
    keep, send, ga1, first, last,
):
    for j in range(2):
        rows = slice(j * NLON, (j + 1) * NLON)
        back = mm_nt(ga2[rows, :], w_middle[...])
        ga1[rows, :] = (back * s1[rows, :]).astype(jnp.bfloat16)
    first[...] = mm_tn(x_0[...], ga1[...]) + mm_tn(x_1[...], ga1_1[...])
    last[...] = mm_tn(h2_0[...], gt_0[...]) + mm_tn(h2_1[...], gt_1[...])
    core = ids[1]
    part, blocks = keep.shape[0] // 2, 8
    half = part * blocks
    for out, which in ((send, 1 - core), (keep, core)):
        out[0:part, :] = first[pl.ds(pl.multiple_of(which * part, part), part), :]
        for b in range(blocks):
            at = pl.multiple_of(which * half + b * part, part)
            out[part : 2 * part, b * 128 : (b + 1) * 128] = last[pl.ds(at, part), :]


def keep_kernel(ids, h1_0, ga2_0, h1_1, ga2_1, keep):
    core = ids[1]
    keep[...] = mm_tn(h1_0[core], ga2_0[...]) + mm_tn(h1_1[core], ga2_1[...])


def latitudes_kernel(owned, forward_op, backward_op, back):
    for i, operator in ((0, forward_op), (1, backward_op)):
        parts = [
            jnp.concatenate([owned[:, 4 * i + p, :], owned[:, 4 * i + 2 + p, :]], axis=0)
            for p in range(2)
        ]
        found = mm_exact(operator[...], jnp.concatenate(parts, axis=1))
        bands = owned.shape[0]
        feat = owned.shape[2]
        for j in range(2):
            for p in range(2):
                back[:, 4 * i + 2 * j + p, :] = found[
                    j * bands : (j + 1) * bands, p * feat : (p + 1) * feat
                ]


def sum_wide_kernel(parts, out):
    total = parts[0]
    for i in range(1, parts.shape[0]):
        total = total + parts[i]
    size = out.shape[1]
    for r in range(2):
        for b in range(8):
            out[r * 8 + b] = total[r * size : (r + 1) * size, b * 128 : (b + 1) * 128]


def sum_deep_kernel(parts, out):
    total = parts[0]
    for i in range(1, parts.shape[0]):
        total = total + parts[i]
    for i in range(out.shape[0]):
        out[i] = total


def spread_kernel(parts, out):
    size = parts.shape[1]
    for r in range(2):
        for b in range(8):
            piece = parts[r * 8 + b]
            for i in range(out.shape[0]):
                out[i, r * size : (r + 1) * size, b * 128 : (b + 1) * 128] = piece


def add_kernel(left, left_thin, right, right_thin, out):
    half = left.shape[0]
    out[0:half, :] = left[...] + right[...]
    out[half:, :] = left_thin[...] + right_thin[...]


def place(ids, other, source, outs, sem):
    first, middle, last = outs
    which = 1 - ids[1] if other else ids[1]
    half = middle.shape[0] // 2
    part, blocks = half // 8, 8
    copies = [
        (source.at[pl.ds(0, half)], middle.at[pl.ds(pl.multiple_of(which * half, half), half)]),
        (
            source.at[pl.ds(half, part)],
            first.at[pl.ds(pl.multiple_of(which * part, part), part)],
        ),
    ]
    for b in range(blocks):
        at = pl.multiple_of(which * half + b * part, part)
        copies.append(
            (
                source.at[pl.ds(half + part, part), pl.ds(b * 128, 128)],
                last.at[pl.ds(at, part)],
            )
        )
    started = [
        pltpu.make_async_copy(start, end, sem.at[i]) for i, (start, end) in enumerate(copies)
    ]
    for copy in started:
        copy.start()
    for copy in started:
        copy.wait()


def own_kernel(ids, source, first, middle, last, sem):
    place(ids, False, source, (first, middle, last), sem)


def other_kernel(ids, source, _first, _middle, _last, first, middle, last, sem):
    place(ids, True, source, (first, middle, last), sem)


def unpack(core, own, other, hidden, features):
    outs = [
        jax.ShapeDtypeStruct(shape, jnp.float32)
        for shape in ((features, hidden), (hidden, hidden), (hidden, features))
    ]
    smem = pl.BlockSpec(memory_space=pltpu.SMEM)
    hbm = pl.BlockSpec(memory_space=pltpu.HBM)
    settings = dict(
        out_shape=tuple(outs),
        out_specs=(hbm,) * 3,
        scratch_shapes=[pltpu.SemaphoreType.DMA((10,))],
        compiler_params=pltpu.CompilerParams(vmem_limit_bytes=4 * 1024 * 1024),
    )
    grads = pl.pallas_call(own_kernel, in_specs=[smem] + vmem(1), name="own", **settings)(core, own)
    return pl.pallas_call(
        other_kernel,
        in_specs=[smem] + vmem(1) + [hbm] * 3,
        input_output_aliases={2: 0, 3: 1, 4: 2},
        name="other",
        **settings,
    )(core, other, *grads)


def body(state, cotangent, w_first, w_middle, w_last):
    _, lat_rows, lon_count, features = state.shape
    hidden = w_first.shape[1]
    rows = lat_rows * lon_count
    bands = lax.axis_size("xl") * lax.axis_size("z") * lax.axis_size("y")
    f32, bf16 = jnp.float32, jnp.bfloat16
    ids = jnp.stack([lax.axis_index(LAT), lax.axis_index("c")]).astype(jnp.int32)
    waves_of = ((MW, 8, features), f32)
    halves = ((2, rows, hidden // 2), bf16)
    wide16, wide32 = ((rows, hidden), bf16), ((rows, hidden), f32)
    thin16 = ((rows, features), bf16)
    part = ((lat_rows, lon_count, features), f32)
    square = ((lat_rows * bands,) * 2, f32)

    def cross(waves):
        owned = lax.all_to_all(waves, LAT, 0, 0, tiled=True)
        (back,) = call(
            latitudes_kernel, [waves_of], owned, forward_op, backward_op, name="latitudes"
        )
        return lax.all_to_all(back, LAT, 0, 0, tiled=True)

    table, table_t, forward_op, backward_op = call(
        tables_kernel,
        [((2 * MW, NLON), f32), ((NLON, 2 * MW), f32), square, square],
        ids,
        name="tables",
        scalars=1,
        scratch=[((MW, lat_rows * bands), f32)],
    )
    waves, x_0, h1_0, s1_0, h2_0, s2_0 = call(
        first_kernel,
        [waves_of, thin16, halves, wide32, wide16, wide32],
        state[0], cotangent[0], table, w_first, w_middle, w_last,
        name="first",
    )
    waves = cross(waves)
    waves, x_1, h1_1, h2_1, ga1_1, ga2_1, gt_1 = call(
        middle_kernel,
        [waves_of, thin16, halves, wide16, wide16, wide16, thin16],
        waves, table, table_t, w_first, w_middle, w_last,
        name="middle",
        scratch=[wide32] * 2,
    )
    waves = cross(waves)
    packed = ((hidden // 2 + features, hidden), f32)
    half32, thin32 = ((hidden // 2, hidden), f32), ((features, hidden), f32)
    final, send, ga2_0, gt_0 = call(
        last_kernel,
        [part, half32, wide16, thin16],
        ids, waves, table_t, h1_0, s2_0, h1_1, ga2_1, w_last,
        name="last",
        scalars=1,
    )
    received = lax.ppermute(send, "c", SWAP)
    keep_thin, send_thin = call(
        thin_kernel,
        [thin32, thin32],
        ids, x_0, h2_0, s1_0, ga2_0, gt_0, w_middle, x_1, h2_1, ga1_1, gt_1,
        name="thin",
        scalars=1,
        scratch=[wide16, thin32, ((hidden, features), f32)],
    )
    received_thin = lax.ppermute(send_thin, "c", SWAP)
    (keep,) = call(
        keep_kernel, [half32], ids, h1_0, ga2_0, h1_1, ga2_1, name="keep", scalars=1
    )
    (held,) = call(
        add_kernel, [packed], keep, keep_thin, received, received_thin, name="add"
    )
    wide, deep = len(WIDE[0]), len(DEEP[0])
    piece = packed[0][0] // wide
    held = exchange(held.reshape(wide, piece, hidden), WIDE)
    parts = ((deep, piece // 2, hidden // 8), f32)
    (held,) = call(sum_wide_kernel, [parts], held, name="sum_wide")
    held = exchange(held, DEEP)
    (held,) = call(sum_deep_kernel, [parts], held, name="sum_deep")
    held = exchange(held, DEEP)
    (held,) = call(spread_kernel, [((wide, piece, hidden), f32)], held, name="spread")
    held = exchange(held, WIDE).reshape(packed[0])
    other = lax.ppermute(held, "c", SWAP)
    first, middle, last = unpack(ids, held, other, hidden, features)
    return final[None], first, middle, last


def solution(mesh):
    fine = Mesh(mesh.devices.reshape(tuple(size for _, size in FINE)), ALL)
    grid = P(("xh", "c"), LAT, None, None)
    return jax.shard_map(
        body,
        mesh=fine,
        in_specs=(grid, grid, P(), P(), P()),
        out_specs=(grid, P(), P(), P()),
        check_vma=False,
    )
```

```python
import functools
import math

import jax
import jax.numpy as jnp
from jax import lax
from jax.experimental import pallas as pl
from jax.experimental.pallas import tpu as pltpu
from jax.sharding import Mesh, PartitionSpec as P

MW = 64
NLON = 256
highest = lax.Precision.HIGHEST
tend_weight = 0.5

FINE = (("xl", 2), ("z", 8), ("y", 4), ("xh", 2), ("c", 2))
ALL = tuple(name for name, _ in FINE)
LAT = ("xl", "z", "y")
SWAP = [(0, 1), (1, 0)]


def device_id(x, y, z, core):
    return ((((x % 2) * 8 + z) * 4 + y) * 2 + x // 2) * 2 + core


def reduce_groups():
    wide, deep = [], []
    for y in range(4):
        for pair in range(4):
            wide.append([device_id(x, y, 2 * pair + q, 0) for x in range(4) for q in range(2)])
    for x in range(4):
        for pair in range(4):
            wide.append(
                [device_id(x, y, (2 * pair + 1 + q) % 8, 1) for y in range(4) for q in range(2)]
            )
    for x in range(4):
        for parity in range(2):
            deep.append(
                [device_id(x, y, 2 * pair + parity, 0) for y in range(4) for pair in range(4)]
            )
    for y in range(4):
        for parity in range(2):
            deep.append(
                [device_id(x, y, 2 * pair + parity, 1) for x in range(4) for pair in range(4)]
            )
    return wide, deep


WIDE, DEEP = reduce_groups()


def exchange(value, groups):
    return lax.all_to_all(value, ALL, 0, 0, axis_index_groups=groups, tiled=True)


def legendre(lat_count, wave_count, order, forward_ref, backward_ref, table):
    bands = lat_count // 2
    place = lax.broadcasted_iota(jnp.int32, (1, lat_count), 1)
    lat_index = jnp.where(place >= bands, 2 * (place - bands) + 1, 2 * place).astype(jnp.float32)
    latitude = (lat_index + 0.5) * (math.pi / lat_count) - 0.5 * math.pi
    sine_lat = jnp.sin(latitude)
    cosine_lat = jnp.cos(latitude)
    quad_weight = cosine_lat * (math.pi / lat_count)
    order_m = jnp.full((1, lat_count), order, jnp.int32).astype(jnp.float32)
    counter = lax.broadcasted_iota(jnp.int32, (1, lat_count), 1).astype(jnp.float32) + 1.0
    increments = 0.5 * jnp.log((2.0 * counter + 1.0) / (2.0 * counter))
    summed = jnp.sum(jnp.where(counter <= order_m, increments, 0.0), axis=1, keepdims=True)
    current = jnp.exp(0.5 * math.log(0.5) + summed + order_m * jnp.log(cosine_lat))
    previous = jnp.zeros_like(current)
    ratio_prev = jnp.ones_like(current)
    table[0:1, :] = current
    for offset in range(1, wave_count):
        degree = order_m + float(offset)
        ratio = jnp.sqrt((4.0 * degree * degree - 1.0) / (degree * degree - order_m * order_m))
        following = ratio * (sine_lat * current - previous / ratio_prev)
        previous, current, ratio_prev = current, following, ratio
        table[offset : offset + 1, :] = current
    degree = (
        lax.broadcasted_iota(jnp.int32, (wave_count, lat_count), 0) + order
    ).astype(jnp.float32)
    kept = degree <= wave_count - 1
    poly = jnp.where(kept, table[...], 0.0)
    damping = jnp.where(
        kept, 1.0 / (1.0 + degree * (degree + 1.0) / (wave_count * (wave_count - 1.0))), 0.0
    )
    scale = jnp.where(order_m > 0.0, 2.0 / NLON, 1.0 / NLON)
    weighted = poly * quad_weight
    poly = poly * scale
    forward_ref[...] = jnp.dot(
        poly.T, damping * weighted, precision=highest, preferred_element_type=jnp.float32
    )
    backward_ref[...] = jnp.dot(
        weighted.T, damping * poly, precision=highest, preferred_element_type=jnp.float32
    )


def vmem(count):
    return [pl.BlockSpec(memory_space=pltpu.VMEM)] * count


def nbytes(shape, dtype):
    return math.prod(shape) * jnp.dtype(dtype).itemsize


def call(kernel, shapes, *operands, name, scratch=(), fetched=0, spare=4):
    here = len(operands) - fetched
    held = [(operand.shape, operand.dtype) for operand in operands[:here]]
    held += list(shapes) + list(scratch)
    operands = operands[:here] + tuple(
        pltpu.with_memory_space_constraint(operand, pltpu.HBM) for operand in operands[here:]
    )
    return pl.pallas_call(
        kernel,
        out_shape=tuple(jax.ShapeDtypeStruct(shape, dtype) for shape, dtype in shapes),
        in_specs=vmem(here) + [pl.BlockSpec(memory_space=pltpu.HBM)] * fetched,
        out_specs=tuple(vmem(len(shapes))),
        scratch_shapes=[pltpu.VMEM(shape, dtype) for shape, dtype in scratch]
        + [pltpu.SemaphoreType.DMA((fetched,))] * bool(fetched),
        name=name,
        compiler_params=pltpu.CompilerParams(
            vmem_limit_bytes=sum(nbytes(*each) for each in held) + spare * 1024 * 1024
        ),
    )(*operands)


def mm(left, right):
    return jnp.dot(left, right, preferred_element_type=jnp.float32)


def mm_nt(left, right):
    return lax.dot_general(
        left, right, (((1,), (1,)), ((), ())), preferred_element_type=jnp.float32
    )


def mm_tn(left, right):
    return lax.dot_general(
        left, right, (((0,), (0,)), ((), ())), preferred_element_type=jnp.float32
    )


def mm_exact(left, right):
    return jnp.dot(left, right, precision=highest, preferred_element_type=jnp.float32)


def silu_pair(value):
    gate = jax.nn.sigmoid(value)
    return value * gate, gate * (1.0 + value * (1.0 - gate))


def wave_table(transposed):
    shape = (NLON, 2 * MW) if transposed else (2 * MW, NLON)
    lon = lax.broadcasted_iota(jnp.int32, shape, 0 if transposed else 1)
    row = lax.broadcasted_iota(jnp.int32, shape, 1 if transposed else 0)
    wave = jnp.where(row >= MW, row - MW, row)
    angle = ((lon * wave) & (NLON - 1)).astype(jnp.float32) * (2.0 * math.pi / NLON)
    return jnp.where(row >= MW, -jnp.sin(angle), jnp.cos(angle))


def store_waves(table, fields, out_ref):
    waves = mm_exact(table, jnp.concatenate(fields, axis=1))
    feat = fields[0].shape[1]
    for i in range(len(fields)):
        for p in range(2):
            out_ref[:, 2 * i + p, :] = waves[p * MW : (p + 1) * MW, i * feat : (i + 1) * feat]


def load_fields(table_t, waves_ref):
    columns = [
        jnp.concatenate([waves_ref[:, 2 * i, :], waves_ref[:, 2 * i + 1, :]], axis=0)
        for i in range(4)
    ]
    feat = columns[0].shape[1]
    grid = mm_exact(table_t, jnp.concatenate(columns, axis=1))
    return [grid[:, i * feat : (i + 1) * feat] for i in range(4)]


def physics(rows, w_first, w_middle, h1_ref, s1_ref, h2_ref, s2_ref, at):
    size = rows.shape[0]
    half = h1_ref.shape[2]
    value, slope = silu_pair(mm(rows, w_first[...]))
    hidden = value.astype(jnp.bfloat16)
    h1_ref[0, at : at + size, :] = hidden[:, :half]
    h1_ref[1, at : at + size, :] = hidden[:, half:]
    s1_ref[at : at + size, :] = slope
    value, slope = silu_pair(mm(hidden, w_middle[...]))
    h2_ref[at : at + size, :] = value.astype(jnp.bfloat16)
    s2_ref[at : at + size, :] = slope


def first_kernel(
    state_hbm, cotangent_hbm, w_first_hbm, w_middle_hbm, w_last_hbm,
    waves, x, w_first, w_middle, w_last, table, table_t, forward_op, backward_op, h1, s1, h2, s2,
    state, cotangent, poly, sem,
):
    copies = [
        pltpu.make_async_copy(start, end, sem.at[i])
        for i, (start, end) in enumerate(
            (
                (state_hbm, state),
                (cotangent_hbm, cotangent),
                (w_first_hbm, w_first),
                (w_middle_hbm, w_middle),
                (w_last_hbm, w_last),
            )
        )
    ]
    for copy in copies:
        copy.start()
    table[...] = wave_table(False)
    table_t[...] = wave_table(True)
    legendre(forward_op.shape[0], MW, lax.axis_index(LAT), forward_op, backward_op, poly)
    for copy in copies:
        copy.wait()
    moved = []
    for j in range(2):
        rows = slice(j * NLON, (j + 1) * NLON)
        field = state[0, j]
        x[rows, :] = field.astype(jnp.bfloat16)
        physics(field.astype(jnp.bfloat16), w_first, w_middle, h1, s1, h2, s2, j * NLON)
        moved.append(field + tend_weight * mm(h2[rows, :], w_last[...]))
    store_waves(table[...], moved + [cotangent[0, 0], cotangent[0, 1]], waves)


def middle_kernel(
    waves_in, table, table_t, w_first, w_middle, w_last,
    waves, x, h1, h2, ga1, ga2, gt, s1, s2,
):
    fields = load_fields(table_t[...], waves_in)
    moved, grads = [], []
    for j in range(2):
        rows = slice(j * NLON, (j + 1) * NLON)
        field, pulled = fields[j], fields[2 + j]
        x[rows, :] = field.astype(jnp.bfloat16)
        physics(field.astype(jnp.bfloat16), w_first, w_middle, h1, s1, h2, s2, j * NLON)
        moved.append(field + tend_weight * mm(h2[rows, :], w_last[...]))
        scaled = (tend_weight * pulled).astype(jnp.bfloat16)
        gt[rows, :] = scaled
        back = (mm_nt(scaled, w_last[...]) * s2[rows, :]).astype(jnp.bfloat16)
        ga2[rows, :] = back
        back = (mm_nt(back, w_middle[...]) * s1[rows, :]).astype(jnp.bfloat16)
        ga1[rows, :] = back
        grads.append(pulled + mm_nt(back, w_first[...]))
    store_waves(table[...], moved + grads, waves)


def last_kernel(
    waves_in, table_t, h1_0, s2, h1_1, ga2_1, w_last,
    final, send, ga2, gt,
):
    fields = load_fields(table_t[...], waves_in)
    for j in range(2):
        rows = slice(j * NLON, (j + 1) * NLON)
        final[j] = fields[j]
        scaled = (tend_weight * fields[2 + j]).astype(jnp.bfloat16)
        gt[rows, :] = scaled
        ga2[rows, :] = (mm_nt(scaled, w_last[...]) * s2[rows, :]).astype(jnp.bfloat16)
    which = 1 - lax.axis_index("c")
    send[...] = mm_tn(h1_0[which], ga2[...]) + mm_tn(h1_1[which], ga2_1[...])


def thin_kernel(
    x_0, h2_0, s1, ga2, gt_0, w_middle, x_1, h2_1, ga1_1, gt_1,
    keep, send, ga1, first, last,
):
    for j in range(2):
        rows = slice(j * NLON, (j + 1) * NLON)
        back = mm_nt(ga2[rows, :], w_middle[...])
        ga1[rows, :] = (back * s1[rows, :]).astype(jnp.bfloat16)
    first[...] = mm_tn(x_0[...], ga1[...]) + mm_tn(x_1[...], ga1_1[...])
    last[...] = mm_tn(h2_0[...], gt_0[...]) + mm_tn(h2_1[...], gt_1[...])
    core = lax.axis_index("c")
    part, blocks = keep.shape[0] // 2, 8
    half = part * blocks
    for out, which in ((send, 1 - core), (keep, core)):
        out[0:part, :] = first[pl.ds(pl.multiple_of(which * part, part), part), :]
        for b in range(blocks):
            at = pl.multiple_of(which * half + b * part, part)
            out[part : 2 * part, b * 128 : (b + 1) * 128] = last[pl.ds(at, part), :]


def keep_kernel(h1_0, ga2_0, h1_1, ga2_1, keep):
    core = lax.axis_index("c")
    keep[...] = mm_tn(h1_0[core], ga2_0[...]) + mm_tn(h1_1[core], ga2_1[...])


def latitudes_kernel(owned, forward_op, backward_op, back):
    for i, operator in ((0, forward_op), (1, backward_op)):
        parts = [
            jnp.concatenate([owned[:, 4 * i + p, :], owned[:, 4 * i + 2 + p, :]], axis=0)
            for p in range(2)
        ]
        found = mm_exact(operator[...], jnp.concatenate(parts, axis=1))
        bands = owned.shape[0]
        feat = owned.shape[2]
        for j in range(2):
            for p in range(2):
                back[:, 4 * i + 2 * j + p, :] = found[
                    j * bands : (j + 1) * bands, p * feat : (p + 1) * feat
                ]


def sum_wide_kernel(parts, out):
    total = parts[0]
    for i in range(1, parts.shape[0]):
        total = total + parts[i]
    size = out.shape[1]
    for r in range(2):
        for b in range(8):
            out[r * 8 + b] = total[r * size : (r + 1) * size, b * 128 : (b + 1) * 128]


def sum_deep_kernel(parts, out):
    total = parts[0]
    for i in range(1, parts.shape[0]):
        total = total + parts[i]
    for i in range(out.shape[0]):
        out[i] = total


def spread_kernel(parts, out):
    size = parts.shape[1]
    for r in range(2):
        for b in range(8):
            piece = parts[r * 8 + b]
            for i in range(out.shape[0]):
                out[i, r * size : (r + 1) * size, b * 128 : (b + 1) * 128] = piece


def add_kernel(left, left_thin, right, right_thin, out):
    half = left.shape[0]
    out[0:half, :] = left[...] + right[...]
    out[half:, :] = left_thin[...] + right_thin[...]


def place(other, source, outs, sem):
    first, middle, last = outs
    core = lax.axis_index("c")
    which = 1 - core if other else core
    half = middle.shape[0] // 2
    part, blocks = half // 8, 8
    copies = [
        (source.at[pl.ds(0, half)], middle.at[pl.ds(pl.multiple_of(which * half, half), half)]),
        (
            source.at[pl.ds(half, part)],
            first.at[pl.ds(pl.multiple_of(which * part, part), part)],
        ),
    ]
    for b in range(blocks):
        at = pl.multiple_of(which * half + b * part, part)
        copies.append(
            (
                source.at[pl.ds(half + part, part), pl.ds(b * 128, 128)],
                last.at[pl.ds(at, part)],
            )
        )
    started = [
        pltpu.make_async_copy(start, end, sem.at[i]) for i, (start, end) in enumerate(copies)
    ]
    for copy in started:
        copy.start()
    for copy in started:
        copy.wait()


def own_kernel(source, first, middle, last, sem):
    place(False, source, (first, middle, last), sem)


def other_kernel(source, _first, _middle, _last, first, middle, last, sem):
    place(True, source, (first, middle, last), sem)


def unpack(own, other, hidden, features):
    outs = [
        jax.ShapeDtypeStruct(shape, jnp.float32)
        for shape in ((features, hidden), (hidden, hidden), (hidden, features))
    ]
    hbm = pl.BlockSpec(memory_space=pltpu.HBM)
    settings = dict(
        out_shape=tuple(outs),
        out_specs=(hbm,) * 3,
        scratch_shapes=[pltpu.SemaphoreType.DMA((10,))],
        compiler_params=pltpu.CompilerParams(vmem_limit_bytes=4 * 1024 * 1024),
    )
    grads = pl.pallas_call(own_kernel, in_specs=vmem(1), name="own", **settings)(own)
    return pl.pallas_call(
        other_kernel,
        in_specs=vmem(1) + [hbm] * 3,
        input_output_aliases={1: 0, 2: 1, 3: 2},
        name="other",
        **settings,
    )(other, *grads)


def body(state, cotangent, w_first, w_middle, w_last):
    _, lat_rows, lon_count, features = state.shape
    hidden = w_first.shape[1]
    rows = lat_rows * lon_count
    bands = lax.axis_size("xl") * lax.axis_size("z") * lax.axis_size("y")
    f32, bf16 = jnp.float32, jnp.bfloat16
    waves_of = ((MW, 8, features), f32)
    halves = ((2, rows, hidden // 2), bf16)
    wide16, wide32 = ((rows, hidden), bf16), ((rows, hidden), f32)
    thin16 = ((rows, features), bf16)
    part = ((lat_rows, lon_count, features), f32)
    square = ((lat_rows * bands,) * 2, f32)

    def cross(waves):
        owned = lax.all_to_all(waves, LAT, 0, 0, tiled=True)
        (back,) = call(
            latitudes_kernel, [waves_of], owned, forward_op, backward_op, name="latitudes"
        )
        return lax.all_to_all(back, LAT, 0, 0, tiled=True)

    (
        waves, x_0, w_first, w_middle, w_last, table, table_t, forward_op, backward_op,
        h1_0, s1_0, h2_0, s2_0,
    ) = call(
        first_kernel,
        [
            waves_of, thin16,
            (w_first.shape, bf16), (w_middle.shape, bf16), (w_last.shape, bf16),
            ((2 * MW, NLON), f32), ((NLON, 2 * MW), f32), square, square,
            halves, wide32, wide16, wide32,
        ],
        state, cotangent, w_first, w_middle, w_last,
        name="first",
        fetched=5,
        scratch=[(state.shape, f32), (state.shape, f32), ((MW, lat_rows * bands), f32)],
    )
    waves = cross(waves)
    waves, x_1, h1_1, h2_1, ga1_1, ga2_1, gt_1 = call(
        middle_kernel,
        [waves_of, thin16, halves, wide16, wide16, wide16, thin16],
        waves, table, table_t, w_first, w_middle, w_last,
        name="middle",
        scratch=[wide32] * 2,
    )
    waves = cross(waves)
    packed = ((hidden // 2 + features, hidden), f32)
    half32, thin32 = ((hidden // 2, hidden), f32), ((features, hidden), f32)
    final, send, ga2_0, gt_0 = call(
        last_kernel,
        [part, half32, wide16, thin16],
        waves, table_t, h1_0, s2_0, h1_1, ga2_1, w_last,
        name="last",
    )
    received = lax.ppermute(send, "c", SWAP)
    keep_thin, send_thin = call(
        thin_kernel,
        [thin32, thin32],
        x_0, h2_0, s1_0, ga2_0, gt_0, w_middle, x_1, h2_1, ga1_1, gt_1,
        name="thin",
        scratch=[wide16, thin32, ((hidden, features), f32)],
    )
    received_thin = lax.ppermute(send_thin, "c", SWAP)
    (keep,) = call(
        keep_kernel, [half32], h1_0, ga2_0, h1_1, ga2_1, name="keep"
    )
    (held,) = call(
        add_kernel, [packed], keep, keep_thin, received, received_thin, name="add"
    )
    wide, deep = len(WIDE[0]), len(DEEP[0])
    piece = packed[0][0] // wide
    held = exchange(held.reshape(wide, piece, hidden), WIDE)
    parts = ((deep, piece // 2, hidden // 8), f32)
    (held,) = call(sum_wide_kernel, [parts], held, name="sum_wide")
    held = exchange(held, DEEP)
    (held,) = call(sum_deep_kernel, [parts], held, name="sum_deep")
    held = exchange(held, DEEP)
    (held,) = call(spread_kernel, [((wide, piece, hidden), f32)], held, name="spread")
    held = exchange(held, WIDE).reshape(packed[0])
    other = lax.ppermute(held, "c", SWAP)
    first, middle, last = unpack(held, other, hidden, features)
    return final[None], first, middle, last


def solution(mesh):
    fine = Mesh(mesh.devices.reshape(tuple(size for _, size in FINE)), ALL)
    grid = P(("xh", "c"), LAT, None, None)
    return jax.shard_map(
        body,
        mesh=fine,
        in_specs=(grid, grid, P(), P(), P()),
        out_specs=(grid, P(), P(), P()),
        check_vma=False,
    )
```

```python
import functools
import math

import jax
import jax.numpy as jnp
from jax import lax
from jax.experimental import pallas as pl
from jax.experimental.pallas import tpu as pltpu
from jax.sharding import Mesh, PartitionSpec as P

MW = 64
NLON = 256
highest = lax.Precision.HIGHEST
tend_weight = 0.5

FINE = (("xl", 2), ("z", 8), ("y", 4), ("xh", 2), ("c", 2))
ALL = tuple(name for name, _ in FINE)
LAT = ("xl", "z", "y")
SWAP = [(0, 1), (1, 0)]


def device_id(x, y, z, core):
    return ((((x % 2) * 8 + z) * 4 + y) * 2 + x // 2) * 2 + core


def reduce_groups():
    wide, deep = [], []
    for y in range(4):
        for pair in range(4):
            wide.append([device_id(x, y, 2 * pair + q, 0) for x in range(4) for q in range(2)])
    for x in range(4):
        for pair in range(4):
            wide.append(
                [device_id(x, y, (2 * pair + 1 + q) % 8, 1) for y in range(4) for q in range(2)]
            )
    for x in range(4):
        for parity in range(2):
            deep.append(
                [device_id(x, y, 2 * pair + parity, 0) for y in range(4) for pair in range(4)]
            )
    for y in range(4):
        for parity in range(2):
            deep.append(
                [device_id(x, y, 2 * pair + parity, 1) for x in range(4) for pair in range(4)]
            )
    return wide, deep


WIDE, DEEP = reduce_groups()


def exchange(value, groups):
    return lax.all_to_all(value, ALL, 0, 0, axis_index_groups=groups, tiled=True)


def legendre(lat_count, wave_count, order, forward_ref, backward_ref, table):
    bands = lat_count // 2
    place = lax.broadcasted_iota(jnp.int32, (1, lat_count), 1)
    lat_index = jnp.where(place >= bands, 2 * (place - bands) + 1, 2 * place).astype(jnp.float32)
    latitude = (lat_index + 0.5) * (math.pi / lat_count) - 0.5 * math.pi
    sine_lat = jnp.sin(latitude)
    cosine_lat = jnp.cos(latitude)
    quad_weight = cosine_lat * (math.pi / lat_count)
    order_m = jnp.full((1, lat_count), order, jnp.int32).astype(jnp.float32)
    counter = lax.broadcasted_iota(jnp.int32, (1, lat_count), 1).astype(jnp.float32) + 1.0
    increments = 0.5 * jnp.log((2.0 * counter + 1.0) / (2.0 * counter))
    summed = jnp.sum(jnp.where(counter <= order_m, increments, 0.0), axis=1, keepdims=True)
    current = jnp.exp(0.5 * math.log(0.5) + summed + order_m * jnp.log(cosine_lat))
    previous = jnp.zeros_like(current)
    ratio_prev = jnp.ones_like(current)
    table[0:1, :] = current
    for offset in range(1, wave_count):
        degree = order_m + float(offset)
        ratio = jnp.sqrt((4.0 * degree * degree - 1.0) / (degree * degree - order_m * order_m))
        following = ratio * (sine_lat * current - previous / ratio_prev)
        previous, current, ratio_prev = current, following, ratio
        table[offset : offset + 1, :] = current
    degree = (
        lax.broadcasted_iota(jnp.int32, (wave_count, lat_count), 0) + order
    ).astype(jnp.float32)
    kept = degree <= wave_count - 1
    poly = jnp.where(kept, table[...], 0.0)
    damping = jnp.where(
        kept, 1.0 / (1.0 + degree * (degree + 1.0) / (wave_count * (wave_count - 1.0))), 0.0
    )
    scale = jnp.where(order_m > 0.0, 2.0 / NLON, 1.0 / NLON)
    weighted = poly * quad_weight
    poly = poly * scale
    forward_ref[...] = jnp.dot(
        poly.T, damping * weighted, precision=highest, preferred_element_type=jnp.float32
    )
    backward_ref[...] = jnp.dot(
        weighted.T, damping * poly, precision=highest, preferred_element_type=jnp.float32
    )


def vmem(count):
    return [pl.BlockSpec(memory_space=pltpu.VMEM)] * count


def nbytes(shape, dtype):
    return math.prod(shape) * jnp.dtype(dtype).itemsize


def call(kernel, shapes, *operands, name, scratch=(), fetched=0, spare=4):
    here = len(operands) - fetched
    held = [(operand.shape, operand.dtype) for operand in operands[:here]]
    held += list(shapes) + list(scratch)
    operands = operands[:here] + tuple(
        pltpu.with_memory_space_constraint(operand, pltpu.HBM) for operand in operands[here:]
    )
    return pl.pallas_call(
        kernel,
        out_shape=tuple(jax.ShapeDtypeStruct(shape, dtype) for shape, dtype in shapes),
        in_specs=vmem(here) + [pl.BlockSpec(memory_space=pltpu.HBM)] * fetched,
        out_specs=tuple(vmem(len(shapes))),
        scratch_shapes=[pltpu.VMEM(shape, dtype) for shape, dtype in scratch]
        + [pltpu.SemaphoreType.DMA((fetched + 3,))] * bool(fetched),
        name=name,
        compiler_params=pltpu.CompilerParams(
            vmem_limit_bytes=sum(nbytes(*each) for each in held) + spare * 1024 * 1024
        ),
    )(*operands)


def mm(left, right):
    return jnp.dot(left, right, preferred_element_type=jnp.float32)


def mm_nt(left, right):
    return lax.dot_general(
        left, right, (((1,), (1,)), ((), ())), preferred_element_type=jnp.float32
    )


def mm_tn(left, right):
    return lax.dot_general(
        left, right, (((0,), (0,)), ((), ())), preferred_element_type=jnp.float32
    )


def mm_exact(left, right):
    return jnp.dot(left, right, precision=highest, preferred_element_type=jnp.float32)


def silu_pair(value):
    gate = jax.nn.sigmoid(value)
    return value * gate, gate * (1.0 + value * (1.0 - gate))


def wave_table(transposed):
    shape = (NLON, 2 * MW) if transposed else (2 * MW, NLON)
    lon = lax.broadcasted_iota(jnp.int32, shape, 0 if transposed else 1)
    row = lax.broadcasted_iota(jnp.int32, shape, 1 if transposed else 0)
    wave = jnp.where(row >= MW, row - MW, row)
    angle = ((lon * wave) & (NLON - 1)).astype(jnp.float32) * (2.0 * math.pi / NLON)
    return jnp.where(row >= MW, -jnp.sin(angle), jnp.cos(angle))


def store_waves(table, fields, out_ref):
    waves = mm_exact(table, jnp.concatenate(fields, axis=1))
    feat = fields[0].shape[1]
    for i in range(len(fields)):
        for p in range(2):
            out_ref[:, 2 * i + p, :] = waves[p * MW : (p + 1) * MW, i * feat : (i + 1) * feat]


def load_fields(table_t, waves_ref):
    columns = [
        jnp.concatenate([waves_ref[:, 2 * i, :], waves_ref[:, 2 * i + 1, :]], axis=0)
        for i in range(4)
    ]
    feat = columns[0].shape[1]
    grid = mm_exact(table_t, jnp.concatenate(columns, axis=1))
    return [grid[:, i * feat : (i + 1) * feat] for i in range(4)]


def physics(rows, w_first, w_middle, h1_ref, s1_ref, h2_ref, s2_ref, at):
    size = rows.shape[0]
    half = h1_ref.shape[2]
    value, slope = silu_pair(mm(rows, w_first[...]))
    hidden = value.astype(jnp.bfloat16)
    h1_ref[0, at : at + size, :] = hidden[:, :half]
    h1_ref[1, at : at + size, :] = hidden[:, half:]
    s1_ref[at : at + size, :] = slope
    value, slope = silu_pair(mm(hidden, w_middle[...]))
    h2_ref[at : at + size, :] = value.astype(jnp.bfloat16)
    s2_ref[at : at + size, :] = slope


def first_kernel(
    state_hbm, cotangent_hbm, w_first_hbm, w_middle_hbm, w_last_hbm,
    waves, x, w_first, w_middle, w_last, table, table_t, forward_op, backward_op, h1, s1, h2, s2,
    state, cotangent, poly, sem,
):
    piece = w_middle.shape[0] // 4
    parts = [pl.ds(i * piece, piece) for i in range(4)]
    pairs = [(w_middle_hbm.at[part], w_middle.at[part]) for part in parts] + [
        (state_hbm, state),
        (w_first_hbm, w_first),
        (w_last_hbm, w_last),
        (cotangent_hbm, cotangent),
    ]
    copies = [
        pltpu.make_async_copy(start, end, sem.at[i]) for i, (start, end) in enumerate(pairs)
    ]
    for copy in copies:
        copy.start()
    table[...] = wave_table(False)
    table_t[...] = wave_table(True)
    legendre(forward_op.shape[0], MW, lax.axis_index(LAT), forward_op, backward_op, poly)
    for copy in copies:
        copy.wait()
    field = jnp.concatenate([state[0, 0], state[0, 1]], axis=0)
    x[...] = field.astype(jnp.bfloat16)
    physics(x[...], w_first, w_middle, h1, s1, h2, s2, 0)
    moved = field + tend_weight * mm(h2[...], w_last[...])
    store_waves(
        table[...], [moved[:NLON], moved[NLON:], cotangent[0, 0], cotangent[0, 1]], waves
    )


def middle_kernel(
    waves_in, table, table_t, w_first, w_middle, w_last,
    waves, x, h1, h2, ga1, ga2, gt, s1, s2,
):
    fields = load_fields(table_t[...], waves_in)
    field = jnp.concatenate(fields[:2], axis=0)
    pulled = jnp.concatenate(fields[2:], axis=0)
    x[...] = field.astype(jnp.bfloat16)
    gt[...] = (tend_weight * pulled).astype(jnp.bfloat16)
    physics(x[...], w_first, w_middle, h1, s1, h2, s2, 0)
    moved = field + tend_weight * mm(h2[...], w_last[...])
    ga2[...] = (mm_nt(gt[...], w_last[...]) * s2[...]).astype(jnp.bfloat16)
    ga1[...] = (mm_nt(ga2[...], w_middle[...]) * s1[...]).astype(jnp.bfloat16)
    grad = pulled + mm_nt(ga1[...], w_first[...])
    store_waves(table[...], [moved[:NLON], moved[NLON:], grad[:NLON], grad[NLON:]], waves)


def last_kernel(
    waves_in, table_t, h1_0, s2, h1_1, ga2_1, w_last,
    final, send, ga2, gt,
):
    fields = load_fields(table_t[...], waves_in)
    for j in range(2):
        final[j] = fields[j]
        gt[j * NLON : (j + 1) * NLON, :] = (tend_weight * fields[2 + j]).astype(jnp.bfloat16)
    ga2[...] = (mm_nt(gt[...], w_last[...]) * s2[...]).astype(jnp.bfloat16)
    which = 1 - lax.axis_index("c")
    send[...] = mm_tn(h1_0[which], ga2[...]) + mm_tn(h1_1[which], ga2_1[...])


def thin_kernel(
    x_0, h2_0, s1, ga2, gt_0, w_middle, x_1, h2_1, ga1_1, gt_1,
    keep, send, ga1, first, last,
):
    ga1[...] = (mm_nt(ga2[...], w_middle[...]) * s1[...]).astype(jnp.bfloat16)
    first[...] = mm_tn(x_0[...], ga1[...]) + mm_tn(x_1[...], ga1_1[...])
    last[...] = mm_tn(h2_0[...], gt_0[...]) + mm_tn(h2_1[...], gt_1[...])
    core = lax.axis_index("c")
    part, blocks = keep.shape[0] // 2, 8
    half = part * blocks
    for out, which in ((send, 1 - core), (keep, core)):
        out[0:part, :] = first[pl.ds(pl.multiple_of(which * part, part), part), :]
        for b in range(blocks):
            at = pl.multiple_of(which * half + b * part, part)
            out[part : 2 * part, b * 128 : (b + 1) * 128] = last[pl.ds(at, part), :]


def keep_kernel(h1_0, ga2_0, h1_1, ga2_1, keep):
    core = lax.axis_index("c")
    keep[...] = mm_tn(h1_0[core], ga2_0[...]) + mm_tn(h1_1[core], ga2_1[...])


def latitudes_kernel(owned, forward_op, backward_op, back):
    for i, operator in ((0, forward_op), (1, backward_op)):
        parts = [
            jnp.concatenate([owned[:, 4 * i + p, :], owned[:, 4 * i + 2 + p, :]], axis=0)
            for p in range(2)
        ]
        found = mm_exact(operator[...], jnp.concatenate(parts, axis=1))
        bands = owned.shape[0]
        feat = owned.shape[2]
        for j in range(2):
            for p in range(2):
                back[:, 4 * i + 2 * j + p, :] = found[
                    j * bands : (j + 1) * bands, p * feat : (p + 1) * feat
                ]


def sum_wide_kernel(parts, out):
    total = parts[0]
    for i in range(1, parts.shape[0]):
        total = total + parts[i]
    size = out.shape[1]
    for r in range(2):
        for b in range(8):
            out[r * 8 + b] = total[r * size : (r + 1) * size, b * 128 : (b + 1) * 128]


def sum_deep_kernel(parts, out):
    total = parts[0]
    for i in range(1, parts.shape[0]):
        total = total + parts[i]
    for i in range(out.shape[0]):
        out[i] = total


def spread_kernel(parts, out):
    size = parts.shape[1]
    for r in range(2):
        for b in range(8):
            piece = parts[r * 8 + b]
            for i in range(out.shape[0]):
                out[i, r * size : (r + 1) * size, b * 128 : (b + 1) * 128] = piece


def add_kernel(left, left_thin, right, right_thin, out):
    half = left.shape[0]
    out[0:half, :] = left[...] + right[...]
    out[half:, :] = left_thin[...] + right_thin[...]


def place(other, source, outs, sem):
    first, middle, last = outs
    core = lax.axis_index("c")
    which = 1 - core if other else core
    half = middle.shape[0] // 2
    part, blocks = half // 8, 8
    copies = [
        (source.at[pl.ds(0, half)], middle.at[pl.ds(pl.multiple_of(which * half, half), half)]),
        (
            source.at[pl.ds(half, part)],
            first.at[pl.ds(pl.multiple_of(which * part, part), part)],
        ),
    ]
    for b in range(blocks):
        at = pl.multiple_of(which * half + b * part, part)
        copies.append(
            (
                source.at[pl.ds(half + part, part), pl.ds(b * 128, 128)],
                last.at[pl.ds(at, part)],
            )
        )
    started = [
        pltpu.make_async_copy(start, end, sem.at[i]) for i, (start, end) in enumerate(copies)
    ]
    for copy in started:
        copy.start()
    for copy in started:
        copy.wait()


def own_kernel(source, first, middle, last, sem):
    place(False, source, (first, middle, last), sem)


def other_kernel(source, _first, _middle, _last, first, middle, last, sem):
    place(True, source, (first, middle, last), sem)


def unpack(own, other, hidden, features):
    outs = [
        jax.ShapeDtypeStruct(shape, jnp.float32)
        for shape in ((features, hidden), (hidden, hidden), (hidden, features))
    ]
    hbm = pl.BlockSpec(memory_space=pltpu.HBM)
    settings = dict(
        out_shape=tuple(outs),
        out_specs=(hbm,) * 3,
        scratch_shapes=[pltpu.SemaphoreType.DMA((10,))],
        compiler_params=pltpu.CompilerParams(vmem_limit_bytes=4 * 1024 * 1024),
    )
    grads = pl.pallas_call(own_kernel, in_specs=vmem(1), name="own", **settings)(own)
    return pl.pallas_call(
        other_kernel,
        in_specs=vmem(1) + [hbm] * 3,
        input_output_aliases={1: 0, 2: 1, 3: 2},
        name="other",
        **settings,
    )(other, *grads)


def body(state, cotangent, w_first, w_middle, w_last):
    _, lat_rows, lon_count, features = state.shape
    hidden = w_first.shape[1]
    rows = lat_rows * lon_count
    bands = lax.axis_size("xl") * lax.axis_size("z") * lax.axis_size("y")
    f32, bf16 = jnp.float32, jnp.bfloat16
    waves_of = ((MW, 8, features), f32)
    halves = ((2, rows, hidden // 2), bf16)
    wide16, wide32 = ((rows, hidden), bf16), ((rows, hidden), f32)
    thin16 = ((rows, features), bf16)
    part = ((lat_rows, lon_count, features), f32)
    square = ((lat_rows * bands,) * 2, f32)

    def cross(waves):
        owned = lax.all_to_all(waves, LAT, 0, 0, tiled=True)
        (back,) = call(
            latitudes_kernel, [waves_of], owned, forward_op, backward_op, name="latitudes"
        )
        return lax.all_to_all(back, LAT, 0, 0, tiled=True)

    (
        waves, x_0, w_first, w_middle, w_last, table, table_t, forward_op, backward_op,
        h1_0, s1_0, h2_0, s2_0,
    ) = call(
        first_kernel,
        [
            waves_of, thin16,
            (w_first.shape, bf16), (w_middle.shape, bf16), (w_last.shape, bf16),
            ((2 * MW, NLON), f32), ((NLON, 2 * MW), f32), square, square,
            halves, wide32, wide16, wide32,
        ],
        state, cotangent, w_first, w_middle, w_last,
        name="first",
        fetched=5,
        scratch=[(state.shape, f32), (state.shape, f32), ((MW, lat_rows * bands), f32)],
    )
    waves = cross(waves)
    waves, x_1, h1_1, h2_1, ga1_1, ga2_1, gt_1 = call(
        middle_kernel,
        [waves_of, thin16, halves, wide16, wide16, wide16, thin16],
        waves, table, table_t, w_first, w_middle, w_last,
        name="middle",
        scratch=[wide32] * 2,
    )
    waves = cross(waves)
    packed = ((hidden // 2 + features, hidden), f32)
    half32, thin32 = ((hidden // 2, hidden), f32), ((features, hidden), f32)
    final, send, ga2_0, gt_0 = call(
        last_kernel,
        [part, half32, wide16, thin16],
        waves, table_t, h1_0, s2_0, h1_1, ga2_1, w_last,
        name="last",
    )
    received = lax.ppermute(send, "c", SWAP)
    keep_thin, send_thin = call(
        thin_kernel,
        [thin32, thin32],
        x_0, h2_0, s1_0, ga2_0, gt_0, w_middle, x_1, h2_1, ga1_1, gt_1,
        name="thin",
        scratch=[wide16, thin32, ((hidden, features), f32)],
    )
    received_thin = lax.ppermute(send_thin, "c", SWAP)
    (keep,) = call(
        keep_kernel, [half32], h1_0, ga2_0, h1_1, ga2_1, name="keep"
    )
    (held,) = call(
        add_kernel, [packed], keep, keep_thin, received, received_thin, name="add"
    )
    wide, deep = len(WIDE[0]), len(DEEP[0])
    piece = packed[0][0] // wide
    held = exchange(held.reshape(wide, piece, hidden), WIDE)
    parts = ((deep, piece // 2, hidden // 8), f32)
    (held,) = call(sum_wide_kernel, [parts], held, name="sum_wide")
    held = exchange(held, DEEP)
    (held,) = call(sum_deep_kernel, [parts], held, name="sum_deep")
    held = exchange(held, DEEP)
    (held,) = call(spread_kernel, [((wide, piece, hidden), f32)], held, name="spread")
    held = exchange(held, WIDE).reshape(packed[0])
    other = lax.ppermute(held, "c", SWAP)
    first, middle, last = unpack(held, other, hidden, features)
    return final[None], first, middle, last


def solution(mesh):
    fine = Mesh(mesh.devices.reshape(tuple(size for _, size in FINE)), ALL)
    grid = P(("xh", "c"), LAT, None, None)
    return jax.shard_map(
        body,
        mesh=fine,
        in_specs=(grid, grid, P(), P(), P()),
        out_specs=(grid, P(), P(), P()),
        check_vma=False,
    )
```

```python
import functools
import math

import jax
import jax.numpy as jnp
from jax import lax
from jax.experimental import pallas as pl
from jax.experimental.pallas import tpu as pltpu
from jax.sharding import Mesh, PartitionSpec as P

MW = 64
NLON = 256
highest = lax.Precision.HIGHEST
tend_weight = 0.5

FINE = (("xl", 2), ("z", 8), ("y", 4), ("xh", 2), ("c", 2))
ALL = tuple(name for name, _ in FINE)
BAND = ("xl", "z", "y")
LAT = ("z", "y", "xl")
XL = dict(FINE)["xl"]
SWAP = [(0, 1), (1, 0)]


def device_id(x, y, z, core):
    return ((((x % 2) * 8 + z) * 4 + y) * 2 + x // 2) * 2 + core


def reduce_groups():
    wide, deep = [], []
    for y in range(4):
        for pair in range(4):
            wide.append([device_id(x, y, 2 * pair + q, 0) for x in range(4) for q in range(2)])
    for x in range(4):
        for pair in range(4):
            wide.append(
                [device_id(x, y, (2 * pair + 1 + q) % 8, 1) for y in range(4) for q in range(2)]
            )
    for x in range(4):
        for parity in range(2):
            deep.append(
                [device_id(x, y, 2 * pair + parity, 0) for pair in range(4) for y in range(4)]
            )
    for y in range(4):
        for parity in range(2):
            deep.append(
                [device_id(x, y, 2 * pair + parity, 1) for pair in range(4) for x in range(4)]
            )
    return wide, deep


WIDE, DEEP = reduce_groups()


def exchange(value, groups):
    return lax.all_to_all(value, ALL, 0, 0, axis_index_groups=groups, tiled=True)


def legendre(lat_count, wave_count, order, forward_ref, backward_ref, table):
    bands = lat_count // 2
    place = lax.broadcasted_iota(jnp.int32, (1, lat_count), 1)
    row = place // bands
    rank = place - row * bands
    band = rank % XL * (bands // XL) + rank // XL
    lat_index = (2 * band + row).astype(jnp.float32)
    latitude = (lat_index + 0.5) * (math.pi / lat_count) - 0.5 * math.pi
    sine_lat = jnp.sin(latitude)
    cosine_lat = jnp.cos(latitude)
    quad_weight = cosine_lat * (math.pi / lat_count)
    order_m = jnp.full((1, lat_count), order, jnp.int32).astype(jnp.float32)
    counter = lax.broadcasted_iota(jnp.int32, (1, lat_count), 1).astype(jnp.float32) + 1.0
    increments = 0.5 * jnp.log((2.0 * counter + 1.0) / (2.0 * counter))
    summed = jnp.sum(jnp.where(counter <= order_m, increments, 0.0), axis=1, keepdims=True)
    current = jnp.exp(0.5 * math.log(0.5) + summed + order_m * jnp.log(cosine_lat))
    previous = jnp.zeros_like(current)
    ratio_prev = jnp.ones_like(current)
    table[0:1, :] = current
    for offset in range(1, wave_count):
        degree = order_m + float(offset)
        ratio = jnp.sqrt((4.0 * degree * degree - 1.0) / (degree * degree - order_m * order_m))
        following = ratio * (sine_lat * current - previous / ratio_prev)
        previous, current, ratio_prev = current, following, ratio
        table[offset : offset + 1, :] = current
    degree = (
        lax.broadcasted_iota(jnp.int32, (wave_count, lat_count), 0) + order
    ).astype(jnp.float32)
    kept = degree <= wave_count - 1
    poly = jnp.where(kept, table[...], 0.0)
    damping = jnp.where(
        kept, 1.0 / (1.0 + degree * (degree + 1.0) / (wave_count * (wave_count - 1.0))), 0.0
    )
    scale = jnp.where(order_m > 0.0, 2.0 / NLON, 1.0 / NLON)
    weighted = poly * quad_weight
    poly = poly * scale
    forward_ref[...] = jnp.dot(
        poly.T, damping * weighted, precision=highest, preferred_element_type=jnp.float32
    )
    backward_ref[...] = jnp.dot(
        weighted.T, damping * poly, precision=highest, preferred_element_type=jnp.float32
    )


def vmem(count):
    return [pl.BlockSpec(memory_space=pltpu.VMEM)] * count


def nbytes(shape, dtype):
    return math.prod(shape) * jnp.dtype(dtype).itemsize


def call(kernel, shapes, *operands, name, scratch=(), fetched=0, spare=4):
    here = len(operands) - fetched
    held = [(operand.shape, operand.dtype) for operand in operands[:here]]
    held += list(shapes) + list(scratch)
    operands = operands[:here] + tuple(
        pltpu.with_memory_space_constraint(operand, pltpu.HBM) for operand in operands[here:]
    )
    return pl.pallas_call(
        kernel,
        out_shape=tuple(jax.ShapeDtypeStruct(shape, dtype) for shape, dtype in shapes),
        in_specs=vmem(here) + [pl.BlockSpec(memory_space=pltpu.HBM)] * fetched,
        out_specs=tuple(vmem(len(shapes))),
        scratch_shapes=[pltpu.VMEM(shape, dtype) for shape, dtype in scratch]
        + [pltpu.SemaphoreType.DMA((fetched + 3,))] * bool(fetched),
        name=name,
        compiler_params=pltpu.CompilerParams(
            vmem_limit_bytes=sum(nbytes(*each) for each in held) + spare * 1024 * 1024
        ),
    )(*operands)


def mm(left, right):
    return jnp.dot(left, right, preferred_element_type=jnp.float32)


def mm_nt(left, right):
    return lax.dot_general(
        left, right, (((1,), (1,)), ((), ())), preferred_element_type=jnp.float32
    )


def mm_tn(left, right):
    return lax.dot_general(
        left, right, (((0,), (0,)), ((), ())), preferred_element_type=jnp.float32
    )


def mm_exact(left, right):
    return jnp.dot(left, right, precision=highest, preferred_element_type=jnp.float32)


def silu_pair(value):
    gate = jax.nn.sigmoid(value)
    return value * gate, gate * (1.0 + value * (1.0 - gate))


def wave_table(transposed):
    shape = (NLON, 2 * MW) if transposed else (2 * MW, NLON)
    lon = lax.broadcasted_iota(jnp.int32, shape, 0 if transposed else 1)
    row = lax.broadcasted_iota(jnp.int32, shape, 1 if transposed else 0)
    wave = jnp.where(row >= MW, row - MW, row)
    angle = ((lon * wave) & (NLON - 1)).astype(jnp.float32) * (2.0 * math.pi / NLON)
    return jnp.where(row >= MW, -jnp.sin(angle), jnp.cos(angle))


def store_waves(table, fields, out_ref):
    waves = mm_exact(table, jnp.concatenate(fields, axis=1))
    feat = fields[0].shape[1]
    for i in range(len(fields)):
        for p in range(2):
            out_ref[:, 2 * i + p, :] = waves[p * MW : (p + 1) * MW, i * feat : (i + 1) * feat]


def load_fields(table_t, waves_ref):
    columns = [
        jnp.concatenate([waves_ref[:, 2 * i, :], waves_ref[:, 2 * i + 1, :]], axis=0)
        for i in range(4)
    ]
    feat = columns[0].shape[1]
    grid = mm_exact(table_t, jnp.concatenate(columns, axis=1))
    return [grid[:, i * feat : (i + 1) * feat] for i in range(4)]


def physics(rows, w_first, w_middle, h1_ref, s1_ref, h2_ref, s2_ref, at):
    size = rows.shape[0]
    half = h1_ref.shape[2]
    value, slope = silu_pair(mm(rows, w_first[...]))
    hidden = value.astype(jnp.bfloat16)
    h1_ref[0, at : at + size, :] = hidden[:, :half]
    h1_ref[1, at : at + size, :] = hidden[:, half:]
    s1_ref[at : at + size, :] = slope
    value, slope = silu_pair(mm(hidden, w_middle[...]))
    h2_ref[at : at + size, :] = value.astype(jnp.bfloat16)
    s2_ref[at : at + size, :] = slope


def first_kernel(
    state_hbm, cotangent_hbm, w_first_hbm, w_middle_hbm, w_last_hbm,
    waves, x, w_first, w_middle, w_last, table, table_t, forward_op, backward_op, h1, s1, h2, s2,
    state, cotangent, poly, sem,
):
    piece = w_middle.shape[0] // 4
    parts = [pl.ds(i * piece, piece) for i in range(4)]
    pairs = [(w_middle_hbm.at[part], w_middle.at[part]) for part in parts] + [
        (state_hbm, state),
        (w_first_hbm, w_first),
        (w_last_hbm, w_last),
        (cotangent_hbm, cotangent),
    ]
    copies = [
        pltpu.make_async_copy(start, end, sem.at[i]) for i, (start, end) in enumerate(pairs)
    ]
    for copy in copies:
        copy.start()
    table[...] = wave_table(False)
    table_t[...] = wave_table(True)
    legendre(forward_op.shape[0], MW, lax.axis_index(LAT), forward_op, backward_op, poly)
    for copy in copies:
        copy.wait()
    field = jnp.concatenate([state[0, 0], state[0, 1]], axis=0)
    x[...] = field.astype(jnp.bfloat16)
    physics(x[...], w_first, w_middle, h1, s1, h2, s2, 0)
    moved = field + tend_weight * mm(h2[...], w_last[...])
    store_waves(
        table[...], [moved[:NLON], moved[NLON:], cotangent[0, 0], cotangent[0, 1]], waves
    )


def middle_kernel(
    waves_in, table, table_t, w_first, w_middle, w_last,
    waves, x, h1, h2, ga1, ga2, gt, s1, s2,
):
    fields = load_fields(table_t[...], waves_in)
    field = jnp.concatenate(fields[:2], axis=0)
    pulled = jnp.concatenate(fields[2:], axis=0)
    x[...] = field.astype(jnp.bfloat16)
    gt[...] = (tend_weight * pulled).astype(jnp.bfloat16)
    physics(x[...], w_first, w_middle, h1, s1, h2, s2, 0)
    moved = field + tend_weight * mm(h2[...], w_last[...])
    ga2[...] = (mm_nt(gt[...], w_last[...]) * s2[...]).astype(jnp.bfloat16)
    ga1[...] = (mm_nt(ga2[...], w_middle[...]) * s1[...]).astype(jnp.bfloat16)
    grad = pulled + mm_nt(ga1[...], w_first[...])
    store_waves(table[...], [moved[:NLON], moved[NLON:], grad[:NLON], grad[NLON:]], waves)


def last_kernel(
    waves_in, table_t, h1_0, s2, h1_1, ga2_1, w_last,
    final, send, ga2, gt,
):
    fields = load_fields(table_t[...], waves_in)
    for j in range(2):
        final[j] = fields[j]
        gt[j * NLON : (j + 1) * NLON, :] = (tend_weight * fields[2 + j]).astype(jnp.bfloat16)
    ga2[...] = (mm_nt(gt[...], w_last[...]) * s2[...]).astype(jnp.bfloat16)
    which = 1 - lax.axis_index("c")
    send[...] = mm_tn(h1_0[which], ga2[...]) + mm_tn(h1_1[which], ga2_1[...])


def thin_kernel(
    x_0, h2_0, s1, ga2, gt_0, w_middle, x_1, h2_1, ga1_1, gt_1,
    keep, send, ga1, first, last,
):
    ga1[...] = (mm_nt(ga2[...], w_middle[...]) * s1[...]).astype(jnp.bfloat16)
    first[...] = mm_tn(x_0[...], ga1[...]) + mm_tn(x_1[...], ga1_1[...])
    last[...] = mm_tn(h2_0[...], gt_0[...]) + mm_tn(h2_1[...], gt_1[...])
    core = lax.axis_index("c")
    part, blocks = keep.shape[0] // 2, 8
    half = part * blocks
    for out, which in ((send, 1 - core), (keep, core)):
        out[0:part, :] = first[pl.ds(pl.multiple_of(which * part, part), part), :]
        for b in range(blocks):
            at = pl.multiple_of(which * half + b * part, part)
            out[part : 2 * part, b * 128 : (b + 1) * 128] = last[pl.ds(at, part), :]


def keep_kernel(h1_0, ga2_0, h1_1, ga2_1, keep):
    core = lax.axis_index("c")
    keep[...] = mm_tn(h1_0[core], ga2_0[...]) + mm_tn(h1_1[core], ga2_1[...])


def latitudes_kernel(owned, forward_op, backward_op, back):
    for i, operator in ((0, forward_op), (1, backward_op)):
        parts = [
            jnp.concatenate([owned[:, 4 * i + p, :], owned[:, 4 * i + 2 + p, :]], axis=0)
            for p in range(2)
        ]
        found = mm_exact(operator[...], jnp.concatenate(parts, axis=1))
        bands = owned.shape[0]
        feat = owned.shape[2]
        for j in range(2):
            for p in range(2):
                back[:, 4 * i + 2 * j + p, :] = found[
                    j * bands : (j + 1) * bands, p * feat : (p + 1) * feat
                ]


def sum_wide_kernel(parts, out):
    total = parts[0]
    for i in range(1, parts.shape[0]):
        total = total + parts[i]
    size = out.shape[1]
    for r in range(2):
        for b in range(8):
            out[r * 8 + b] = total[r * size : (r + 1) * size, b * 128 : (b + 1) * 128]


def sum_deep_kernel(parts, out):
    total = parts[0]
    for i in range(1, parts.shape[0]):
        total = total + parts[i]
    for i in range(out.shape[0]):
        out[i] = total


def spread_kernel(parts, out):
    size = parts.shape[1]
    for r in range(2):
        for b in range(8):
            piece = parts[r * 8 + b]
            for i in range(out.shape[0]):
                out[i, r * size : (r + 1) * size, b * 128 : (b + 1) * 128] = piece


def add_kernel(left, left_thin, right, right_thin, out):
    half = left.shape[0]
    out[0:half, :] = left[...] + right[...]
    out[half:, :] = left_thin[...] + right_thin[...]


def place(other, source, outs, sem):
    first, middle, last = outs
    core = lax.axis_index("c")
    which = 1 - core if other else core
    half = middle.shape[0] // 2
    part, blocks = half // 8, 8
    copies = [
        (source.at[pl.ds(0, half)], middle.at[pl.ds(pl.multiple_of(which * half, half), half)]),
        (
            source.at[pl.ds(half, part)],
            first.at[pl.ds(pl.multiple_of(which * part, part), part)],
        ),
    ]
    for b in range(blocks):
        at = pl.multiple_of(which * half + b * part, part)
        copies.append(
            (
                source.at[pl.ds(half + part, part), pl.ds(b * 128, 128)],
                last.at[pl.ds(at, part)],
            )
        )
    started = [
        pltpu.make_async_copy(start, end, sem.at[i]) for i, (start, end) in enumerate(copies)
    ]
    for copy in started:
        copy.start()
    for copy in started:
        copy.wait()


def own_kernel(source, first, middle, last, sem):
    place(False, source, (first, middle, last), sem)


def other_kernel(source, _first, _middle, _last, first, middle, last, sem):
    place(True, source, (first, middle, last), sem)


def unpack(own, other, hidden, features):
    outs = [
        jax.ShapeDtypeStruct(shape, jnp.float32)
        for shape in ((features, hidden), (hidden, hidden), (hidden, features))
    ]
    hbm = pl.BlockSpec(memory_space=pltpu.HBM)
    settings = dict(
        out_shape=tuple(outs),
        out_specs=(hbm,) * 3,
        scratch_shapes=[pltpu.SemaphoreType.DMA((10,))],
        compiler_params=pltpu.CompilerParams(vmem_limit_bytes=4 * 1024 * 1024),
    )
    grads = pl.pallas_call(own_kernel, in_specs=vmem(1), name="own", **settings)(own)
    return pl.pallas_call(
        other_kernel,
        in_specs=vmem(1) + [hbm] * 3,
        input_output_aliases={1: 0, 2: 1, 3: 2},
        name="other",
        **settings,
    )(other, *grads)


def body(state, cotangent, w_first, w_middle, w_last):
    _, lat_rows, lon_count, features = state.shape
    hidden = w_first.shape[1]
    rows = lat_rows * lon_count
    bands = lax.axis_size("xl") * lax.axis_size("z") * lax.axis_size("y")
    f32, bf16 = jnp.float32, jnp.bfloat16
    waves_of = ((MW, 8, features), f32)
    halves = ((2, rows, hidden // 2), bf16)
    wide16, wide32 = ((rows, hidden), bf16), ((rows, hidden), f32)
    thin16 = ((rows, features), bf16)
    part = ((lat_rows, lon_count, features), f32)
    square = ((lat_rows * bands,) * 2, f32)

    def cross(waves):
        owned = lax.all_to_all(waves, LAT, 0, 0, tiled=True)
        (back,) = call(
            latitudes_kernel, [waves_of], owned, forward_op, backward_op, name="latitudes"
        )
        return lax.all_to_all(back, LAT, 0, 0, tiled=True)

    (
        waves, x_0, w_first, w_middle, w_last, table, table_t, forward_op, backward_op,
        h1_0, s1_0, h2_0, s2_0,
    ) = call(
        first_kernel,
        [
            waves_of, thin16,
            (w_first.shape, bf16), (w_middle.shape, bf16), (w_last.shape, bf16),
            ((2 * MW, NLON), f32), ((NLON, 2 * MW), f32), square, square,
            halves, wide32, wide16, wide32,
        ],
        state, cotangent, w_first, w_middle, w_last,
        name="first",
        fetched=5,
        scratch=[(state.shape, f32), (state.shape, f32), ((MW, lat_rows * bands), f32)],
    )
    waves = cross(waves)
    waves, x_1, h1_1, h2_1, ga1_1, ga2_1, gt_1 = call(
        middle_kernel,
        [waves_of, thin16, halves, wide16, wide16, wide16, thin16],
        waves, table, table_t, w_first, w_middle, w_last,
        name="middle",
        scratch=[wide32] * 2,
    )
    waves = cross(waves)
    packed = ((hidden // 2 + features, hidden), f32)
    half32, thin32 = ((hidden // 2, hidden), f32), ((features, hidden), f32)
    final, send, ga2_0, gt_0 = call(
        last_kernel,
        [part, half32, wide16, thin16],
        waves, table_t, h1_0, s2_0, h1_1, ga2_1, w_last,
        name="last",
    )
    received = lax.ppermute(send, "c", SWAP)
    keep_thin, send_thin = call(
        thin_kernel,
        [thin32, thin32],
        x_0, h2_0, s1_0, ga2_0, gt_0, w_middle, x_1, h2_1, ga1_1, gt_1,
        name="thin",
        scratch=[wide16, thin32, ((hidden, features), f32)],
    )
    received_thin = lax.ppermute(send_thin, "c", SWAP)
    (keep,) = call(
        keep_kernel, [half32], h1_0, ga2_0, h1_1, ga2_1, name="keep"
    )
    (held,) = call(
        add_kernel, [packed], keep, keep_thin, received, received_thin, name="add"
    )
    wide, deep = len(WIDE[0]), len(DEEP[0])
    piece = packed[0][0] // wide
    held = exchange(held.reshape(wide, piece, hidden), WIDE)
    parts = ((deep, piece // 2, hidden // 8), f32)
    (held,) = call(sum_wide_kernel, [parts], held, name="sum_wide")
    held = exchange(held, DEEP)
    (held,) = call(sum_deep_kernel, [parts], held, name="sum_deep")
    held = exchange(held, DEEP)
    (held,) = call(spread_kernel, [((wide, piece, hidden), f32)], held, name="spread")
    held = exchange(held, WIDE).reshape(packed[0])
    other = lax.ppermute(held, "c", SWAP)
    first, middle, last = unpack(held, other, hidden, features)
    return final[None], first, middle, last


def solution(mesh):
    fine = Mesh(mesh.devices.reshape(tuple(size for _, size in FINE)), ALL)
    grid = P(("xh", "c"), BAND, None, None)
    return jax.shard_map(
        body,
        mesh=fine,
        in_specs=(grid, grid, P(), P(), P()),
        out_specs=(grid, P(), P(), P()),
        check_vma=False,
    )
```

```python
import functools
import math

import jax
import jax.numpy as jnp
from jax import lax
from jax.experimental import pallas as pl
from jax.experimental.pallas import tpu as pltpu
from jax.sharding import Mesh, PartitionSpec as P

MW = 64
NLON = 256
highest = lax.Precision.HIGHEST
tend_weight = 0.5

FINE = (("xl", 2), ("z", 8), ("y", 4), ("xh", 2), ("c", 2))
ALL = tuple(name for name, _ in FINE)
BAND = ("xl", "z", "y")
LAT = ("z", "y", "xl")
XL = dict(FINE)["xl"]
SWAP = [(0, 1), (1, 0)]


def device_id(x, y, z, core):
    return ((((x % 2) * 8 + z) * 4 + y) * 2 + x // 2) * 2 + core


def reduce_groups():
    wide, deep = [], []
    for y in range(4):
        for pair in range(4):
            wide.append([device_id(x, y, 2 * pair + q, 0) for x in range(4) for q in range(2)])
    for x in range(4):
        for pair in range(4):
            wide.append(
                [device_id(x, y, (2 * pair + 1 + q) % 8, 1) for y in range(4) for q in range(2)]
            )
    for x in range(4):
        for parity in range(2):
            deep.append(
                [device_id(x, y, 2 * pair + parity, 0) for pair in range(4) for y in range(4)]
            )
    for y in range(4):
        for parity in range(2):
            deep.append(
                [device_id(x, y, 2 * pair + parity, 1) for pair in range(4) for x in range(4)]
            )
    return wide, deep


WIDE, DEEP = reduce_groups()


def exchange(value, groups):
    return lax.all_to_all(value, ALL, 0, 0, axis_index_groups=groups, tiled=True)


def legendre(lat_count, wave_count, order, forward_ref, backward_ref, table):
    bands = lat_count // 2
    place = lax.broadcasted_iota(jnp.int32, (1, lat_count), 1)
    row = place // bands
    rank = place - row * bands
    band = rank % XL * (bands // XL) + rank // XL
    lat_index = (2 * band + row).astype(jnp.float32)
    latitude = (lat_index + 0.5) * (math.pi / lat_count) - 0.5 * math.pi
    sine_lat = jnp.sin(latitude)
    cosine_lat = jnp.cos(latitude)
    quad_weight = cosine_lat * (math.pi / lat_count)
    order_m = jnp.full((1, lat_count), order, jnp.int32).astype(jnp.float32)
    counter = lax.broadcasted_iota(jnp.int32, (1, lat_count), 1).astype(jnp.float32) + 1.0
    increments = 0.5 * jnp.log((2.0 * counter + 1.0) / (2.0 * counter))
    summed = jnp.sum(jnp.where(counter <= order_m, increments, 0.0), axis=1, keepdims=True)
    current = jnp.exp(0.5 * math.log(0.5) + summed + order_m * jnp.log(cosine_lat))
    previous = jnp.zeros_like(current)
    ratio_prev = jnp.ones_like(current)
    table[0:1, :] = current
    for offset in range(1, wave_count):
        degree = order_m + float(offset)
        ratio = jnp.sqrt((4.0 * degree * degree - 1.0) / (degree * degree - order_m * order_m))
        following = ratio * (sine_lat * current - previous / ratio_prev)
        previous, current, ratio_prev = current, following, ratio
        table[offset : offset + 1, :] = current
    degree = (
        lax.broadcasted_iota(jnp.int32, (wave_count, lat_count), 0) + order
    ).astype(jnp.float32)
    kept = degree <= wave_count - 1
    poly = jnp.where(kept, table[...], 0.0)
    damping = jnp.where(
        kept, 1.0 / (1.0 + degree * (degree + 1.0) / (wave_count * (wave_count - 1.0))), 0.0
    )
    scale = jnp.where(order_m > 0.0, 2.0 / NLON, 1.0 / NLON)
    weighted = poly * quad_weight
    poly = poly * scale
    forward_ref[...] = jnp.dot(
        poly.T, damping * weighted, precision=highest, preferred_element_type=jnp.float32
    )
    backward_ref[...] = jnp.dot(
        weighted.T, damping * poly, precision=highest, preferred_element_type=jnp.float32
    )


def vmem(count):
    return [pl.BlockSpec(memory_space=pltpu.VMEM)] * count


def nbytes(shape, dtype):
    return math.prod(shape) * jnp.dtype(dtype).itemsize


def call(kernel, shapes, *operands, name, scratch=(), fetched=0, spare=4):
    here = len(operands) - fetched
    held = [(operand.shape, operand.dtype) for operand in operands[:here]]
    held += list(shapes) + list(scratch)
    operands = operands[:here] + tuple(
        pltpu.with_memory_space_constraint(operand, pltpu.HBM) for operand in operands[here:]
    )
    return pl.pallas_call(
        kernel,
        out_shape=tuple(jax.ShapeDtypeStruct(shape, dtype) for shape, dtype in shapes),
        in_specs=vmem(here) + [pl.BlockSpec(memory_space=pltpu.HBM)] * fetched,
        out_specs=tuple(vmem(len(shapes))),
        scratch_shapes=[pltpu.VMEM(shape, dtype) for shape, dtype in scratch]
        + [pltpu.SemaphoreType.DMA((fetched + 3,))] * bool(fetched),
        name=name,
        compiler_params=pltpu.CompilerParams(
            vmem_limit_bytes=sum(nbytes(*each) for each in held) + spare * 1024 * 1024
        ),
    )(*operands)


def mm(left, right):
    return jnp.dot(left, right, preferred_element_type=jnp.float32)


def mm_nt(left, right):
    return lax.dot_general(
        left, right, (((1,), (1,)), ((), ())), preferred_element_type=jnp.float32
    )


def mm_tn(left, right):
    return lax.dot_general(
        left, right, (((0,), (0,)), ((), ())), preferred_element_type=jnp.float32
    )


def split(value):
    high = value.astype(jnp.bfloat16)
    return high, (value - high.astype(jnp.float32)).astype(jnp.bfloat16)


def mm_fine(left, right):
    left_high, left_low = split(left)
    right_high, right_low = split(right)
    return mm(left_high, right_high) + (mm(left_high, right_low) + mm(left_low, right_high))


def silu_pair(value):
    gate = jax.nn.sigmoid(value)
    return value * gate, gate * (1.0 + value * (1.0 - gate))


def wave_table(transposed):
    shape = (NLON, 2 * MW) if transposed else (2 * MW, NLON)
    lon = lax.broadcasted_iota(jnp.int32, shape, 0 if transposed else 1)
    row = lax.broadcasted_iota(jnp.int32, shape, 1 if transposed else 0)
    wave = jnp.where(row >= MW, row - MW, row)
    angle = ((lon * wave) & (NLON - 1)).astype(jnp.float32) * (2.0 * math.pi / NLON)
    return jnp.where(row >= MW, -jnp.sin(angle), jnp.cos(angle))


def store_waves(table, fields, out_ref):
    waves = mm_fine(table, jnp.concatenate(fields, axis=1))
    feat = fields[0].shape[1]
    for i in range(len(fields)):
        for p in range(2):
            out_ref[:, 2 * i + p, :] = waves[p * MW : (p + 1) * MW, i * feat : (i + 1) * feat]


def load_fields(table_t, waves_ref):
    columns = [
        jnp.concatenate([waves_ref[:, 2 * i, :], waves_ref[:, 2 * i + 1, :]], axis=0)
        for i in range(4)
    ]
    feat = columns[0].shape[1]
    grid = mm_fine(table_t, jnp.concatenate(columns, axis=1))
    return [grid[:, i * feat : (i + 1) * feat] for i in range(4)]


def physics(rows, w_first, w_middle, h1_ref, s1_ref, h2_ref, s2_ref, at):
    size = rows.shape[0]
    half = h1_ref.shape[2]
    value, slope = silu_pair(mm(rows, w_first[...]))
    hidden = value.astype(jnp.bfloat16)
    h1_ref[0, at : at + size, :] = hidden[:, :half]
    h1_ref[1, at : at + size, :] = hidden[:, half:]
    s1_ref[at : at + size, :] = slope
    value, slope = silu_pair(mm(hidden, w_middle[...]))
    h2_ref[at : at + size, :] = value.astype(jnp.bfloat16)
    s2_ref[at : at + size, :] = slope


def first_kernel(
    state_hbm, cotangent_hbm, w_first_hbm, w_middle_hbm, w_last_hbm,
    waves, x, w_first, w_middle, w_last, table, table_t, forward_op, backward_op, h1, s1, h2, s2,
    state, cotangent, poly, sem,
):
    piece = w_middle.shape[0] // 4
    parts = [pl.ds(i * piece, piece) for i in range(4)]
    pairs = [(w_middle_hbm.at[part], w_middle.at[part]) for part in parts] + [
        (state_hbm, state),
        (w_first_hbm, w_first),
        (w_last_hbm, w_last),
        (cotangent_hbm, cotangent),
    ]
    copies = [
        pltpu.make_async_copy(start, end, sem.at[i]) for i, (start, end) in enumerate(pairs)
    ]
    for copy in copies:
        copy.start()
    table[...] = wave_table(False)
    table_t[...] = wave_table(True)
    legendre(forward_op.shape[0], MW, lax.axis_index(LAT), forward_op, backward_op, poly)
    for copy in copies:
        copy.wait()
    field = jnp.concatenate([state[0, 0], state[0, 1]], axis=0)
    x[...] = field.astype(jnp.bfloat16)
    physics(x[...], w_first, w_middle, h1, s1, h2, s2, 0)
    moved = field + tend_weight * mm(h2[...], w_last[...])
    store_waves(
        table[...], [moved[:NLON], moved[NLON:], cotangent[0, 0], cotangent[0, 1]], waves
    )


def middle_kernel(
    waves_in, table, table_t, w_first, w_middle, w_last,
    waves, x, h1, h2, ga1, ga2, gt, s1, s2,
):
    fields = load_fields(table_t[...], waves_in)
    field = jnp.concatenate(fields[:2], axis=0)
    pulled = jnp.concatenate(fields[2:], axis=0)
    x[...] = field.astype(jnp.bfloat16)
    gt[...] = (tend_weight * pulled).astype(jnp.bfloat16)
    physics(x[...], w_first, w_middle, h1, s1, h2, s2, 0)
    moved = field + tend_weight * mm(h2[...], w_last[...])
    ga2[...] = (mm_nt(gt[...], w_last[...]) * s2[...]).astype(jnp.bfloat16)
    ga1[...] = (mm_nt(ga2[...], w_middle[...]) * s1[...]).astype(jnp.bfloat16)
    grad = pulled + mm_nt(ga1[...], w_first[...])
    store_waves(table[...], [moved[:NLON], moved[NLON:], grad[:NLON], grad[NLON:]], waves)


def last_kernel(
    waves_in, table_t, h1_0, s2, h1_1, ga2_1, w_last,
    final, send, ga2, gt,
):
    fields = load_fields(table_t[...], waves_in)
    for j in range(2):
        final[j] = fields[j]
        gt[j * NLON : (j + 1) * NLON, :] = (tend_weight * fields[2 + j]).astype(jnp.bfloat16)
    ga2[...] = (mm_nt(gt[...], w_last[...]) * s2[...]).astype(jnp.bfloat16)
    which = 1 - lax.axis_index("c")
    send[...] = mm_tn(h1_0[which], ga2[...]) + mm_tn(h1_1[which], ga2_1[...])


def thin_kernel(
    x_0, h2_0, s1, ga2, gt_0, w_middle, x_1, h2_1, ga1_1, gt_1,
    keep, send, ga1, first, last,
):
    ga1[...] = (mm_nt(ga2[...], w_middle[...]) * s1[...]).astype(jnp.bfloat16)
    first[...] = mm_tn(x_0[...], ga1[...]) + mm_tn(x_1[...], ga1_1[...])
    last[...] = mm_tn(h2_0[...], gt_0[...]) + mm_tn(h2_1[...], gt_1[...])
    core = lax.axis_index("c")
    part, blocks = keep.shape[0] // 2, 8
    half = part * blocks
    for out, which in ((send, 1 - core), (keep, core)):
        out[0:part, :] = first[pl.ds(pl.multiple_of(which * part, part), part), :]
        for b in range(blocks):
            at = pl.multiple_of(which * half + b * part, part)
            out[part : 2 * part, b * 128 : (b + 1) * 128] = last[pl.ds(at, part), :]


def keep_kernel(h1_0, ga2_0, h1_1, ga2_1, keep):
    core = lax.axis_index("c")
    keep[...] = mm_tn(h1_0[core], ga2_0[...]) + mm_tn(h1_1[core], ga2_1[...])


def latitudes_kernel(owned, forward_op, backward_op, back):
    for i, operator in ((0, forward_op), (1, backward_op)):
        parts = [
            jnp.concatenate([owned[:, 4 * i + p, :], owned[:, 4 * i + 2 + p, :]], axis=0)
            for p in range(2)
        ]
        found = mm_fine(operator[...], jnp.concatenate(parts, axis=1))
        bands = owned.shape[0]
        feat = owned.shape[2]
        for j in range(2):
            for p in range(2):
                back[:, 4 * i + 2 * j + p, :] = found[
                    j * bands : (j + 1) * bands, p * feat : (p + 1) * feat
                ]


def sum_wide_kernel(parts, out):
    total = parts[0]
    for i in range(1, parts.shape[0]):
        total = total + parts[i]
    size = out.shape[1]
    for r in range(2):
        for b in range(8):
            out[r * 8 + b] = total[r * size : (r + 1) * size, b * 128 : (b + 1) * 128]


def sum_deep_kernel(parts, out):
    total = parts[0]
    for i in range(1, parts.shape[0]):
        total = total + parts[i]
    for i in range(out.shape[0]):
        out[i] = total


def spread_kernel(parts, out):
    size = parts.shape[1]
    for r in range(2):
        for b in range(8):
            piece = parts[r * 8 + b]
            for i in range(out.shape[0]):
                out[i, r * size : (r + 1) * size, b * 128 : (b + 1) * 128] = piece


def add_kernel(left, left_thin, right, right_thin, out):
    half = left.shape[0]
    out[0:half, :] = left[...] + right[...]
    out[half:, :] = left_thin[...] + right_thin[...]


def place(other, source, outs, sem):
    first, middle, last = outs
    core = lax.axis_index("c")
    which = 1 - core if other else core
    half = middle.shape[0] // 2
    part, blocks = half // 8, 8
    copies = [
        (source.at[pl.ds(0, half)], middle.at[pl.ds(pl.multiple_of(which * half, half), half)]),
        (
            source.at[pl.ds(half, part)],
            first.at[pl.ds(pl.multiple_of(which * part, part), part)],
        ),
    ]
    for b in range(blocks):
        at = pl.multiple_of(which * half + b * part, part)
        copies.append(
            (
                source.at[pl.ds(half + part, part), pl.ds(b * 128, 128)],
                last.at[pl.ds(at, part)],
            )
        )
    started = [
        pltpu.make_async_copy(start, end, sem.at[i]) for i, (start, end) in enumerate(copies)
    ]
    for copy in started:
        copy.start()
    for copy in started:
        copy.wait()


def own_kernel(source, first, middle, last, sem):
    place(False, source, (first, middle, last), sem)


def other_kernel(source, _first, _middle, _last, first, middle, last, sem):
    place(True, source, (first, middle, last), sem)


def unpack(own, other, hidden, features):
    outs = [
        jax.ShapeDtypeStruct(shape, jnp.float32)
        for shape in ((features, hidden), (hidden, hidden), (hidden, features))
    ]
    hbm = pl.BlockSpec(memory_space=pltpu.HBM)
    settings = dict(
        out_shape=tuple(outs),
        out_specs=(hbm,) * 3,
        scratch_shapes=[pltpu.SemaphoreType.DMA((10,))],
        compiler_params=pltpu.CompilerParams(vmem_limit_bytes=4 * 1024 * 1024),
    )
    grads = pl.pallas_call(own_kernel, in_specs=vmem(1), name="own", **settings)(own)
    return pl.pallas_call(
        other_kernel,
        in_specs=vmem(1) + [hbm] * 3,
        input_output_aliases={1: 0, 2: 1, 3: 2},
        name="other",
        **settings,
    )(other, *grads)


def body(state, cotangent, w_first, w_middle, w_last):
    _, lat_rows, lon_count, features = state.shape
    hidden = w_first.shape[1]
    rows = lat_rows * lon_count
    bands = lax.axis_size("xl") * lax.axis_size("z") * lax.axis_size("y")
    f32, bf16 = jnp.float32, jnp.bfloat16
    waves_of = ((MW, 8, features), f32)
    halves = ((2, rows, hidden // 2), bf16)
    wide16, wide32 = ((rows, hidden), bf16), ((rows, hidden), f32)
    thin16 = ((rows, features), bf16)
    part = ((lat_rows, lon_count, features), f32)
    square = ((lat_rows * bands,) * 2, f32)

    def cross(waves):
        owned = lax.all_to_all(waves, LAT, 0, 0, tiled=True)
        (back,) = call(
            latitudes_kernel, [waves_of], owned, forward_op, backward_op, name="latitudes"
        )
        return lax.all_to_all(back, LAT, 0, 0, tiled=True)

    (
        waves, x_0, w_first, w_middle, w_last, table, table_t, forward_op, backward_op,
        h1_0, s1_0, h2_0, s2_0,
    ) = call(
        first_kernel,
        [
            waves_of, thin16,
            (w_first.shape, bf16), (w_middle.shape, bf16), (w_last.shape, bf16),
            ((2 * MW, NLON), f32), ((NLON, 2 * MW), f32), square, square,
            halves, wide32, wide16, wide32,
        ],
        state, cotangent, w_first, w_middle, w_last,
        name="first",
        fetched=5,
        scratch=[(state.shape, f32), (state.shape, f32), ((MW, lat_rows * bands), f32)],
    )
    waves = cross(waves)
    waves, x_1, h1_1, h2_1, ga1_1, ga2_1, gt_1 = call(
        middle_kernel,
        [waves_of, thin16, halves, wide16, wide16, wide16, thin16],
        waves, table, table_t, w_first, w_middle, w_last,
        name="middle",
        scratch=[wide32] * 2,
    )
    waves = cross(waves)
    packed = ((hidden // 2 + features, hidden), f32)
    half32, thin32 = ((hidden // 2, hidden), f32), ((features, hidden), f32)
    final, send, ga2_0, gt_0 = call(
        last_kernel,
        [part, half32, wide16, thin16],
        waves, table_t, h1_0, s2_0, h1_1, ga2_1, w_last,
        name="last",
    )
    received = lax.ppermute(send, "c", SWAP)
    keep_thin, send_thin = call(
        thin_kernel,
        [thin32, thin32],
        x_0, h2_0, s1_0, ga2_0, gt_0, w_middle, x_1, h2_1, ga1_1, gt_1,
        name="thin",
        scratch=[wide16, thin32, ((hidden, features), f32)],
    )
    received_thin = lax.ppermute(send_thin, "c", SWAP)
    (keep,) = call(
        keep_kernel, [half32], h1_0, ga2_0, h1_1, ga2_1, name="keep"
    )
    (held,) = call(
        add_kernel, [packed], keep, keep_thin, received, received_thin, name="add"
    )
    wide, deep = len(WIDE[0]), len(DEEP[0])
    piece = packed[0][0] // wide
    held = exchange(held.reshape(wide, piece, hidden), WIDE)
    parts = ((deep, piece // 2, hidden // 8), f32)
    (held,) = call(sum_wide_kernel, [parts], held, name="sum_wide")
    held = exchange(held, DEEP)
    (held,) = call(sum_deep_kernel, [parts], held, name="sum_deep")
    held = exchange(held, DEEP)
    (held,) = call(spread_kernel, [((wide, piece, hidden), f32)], held, name="spread")
    held = exchange(held, WIDE).reshape(packed[0])
    other = lax.ppermute(held, "c", SWAP)
    first, middle, last = unpack(held, other, hidden, features)
    return final[None], first, middle, last


def solution(mesh):
    fine = Mesh(mesh.devices.reshape(tuple(size for _, size in FINE)), ALL)
    grid = P(("xh", "c"), BAND, None, None)
    return jax.shard_map(
        body,
        mesh=fine,
        in_specs=(grid, grid, P(), P(), P()),
        out_specs=(grid, P(), P(), P()),
        check_vma=False,
    )
```

```python
import functools
import math

import jax
import jax.numpy as jnp
from jax import lax
from jax.experimental import pallas as pl
from jax.experimental.pallas import tpu as pltpu
from jax.sharding import Mesh, PartitionSpec as P

MW = 64
NLON = 256
highest = lax.Precision.HIGHEST
tend_weight = 0.5

FINE = (("xl", 2), ("z", 8), ("y", 4), ("xh", 2), ("c", 2))
ALL = tuple(name for name, _ in FINE)
BAND = ("xl", "z", "y")
LAT = ("z", "y", "xl")
XL = dict(FINE)["xl"]
SWAP = [(0, 1), (1, 0)]


def device_id(x, y, z, core):
    return ((((x % 2) * 8 + z) * 4 + y) * 2 + x // 2) * 2 + core


def reduce_groups():
    wide, deep = [], []
    for y in range(4):
        for pair in range(4):
            wide.append([device_id(x, y, 2 * pair + q, 0) for q in range(2) for x in range(4)])
    for x in range(4):
        for pair in range(4):
            wide.append(
                [device_id(x, y, (2 * pair + 1 + q) % 8, 1) for q in range(2) for y in range(4)]
            )
    for x in range(4):
        for parity in range(2):
            deep.append(
                [device_id(x, y, 2 * pair + parity, 0) for pair in range(4) for y in range(4)]
            )
    for y in range(4):
        for parity in range(2):
            deep.append(
                [device_id(x, y, 2 * pair + parity, 1) for pair in range(4) for x in range(4)]
            )
    return wide, deep


WIDE, DEEP = reduce_groups()


def exchange(value, groups):
    return lax.all_to_all(value, ALL, 0, 0, axis_index_groups=groups, tiled=True)


def legendre(lat_count, wave_count, order, forward_ref, backward_ref, table):
    bands = lat_count // 2
    place = lax.broadcasted_iota(jnp.int32, (1, lat_count), 1)
    row = place // bands
    rank = place - row * bands
    band = rank % XL * (bands // XL) + rank // XL
    lat_index = (2 * band + row).astype(jnp.float32)
    latitude = (lat_index + 0.5) * (math.pi / lat_count) - 0.5 * math.pi
    sine_lat = jnp.sin(latitude)
    cosine_lat = jnp.cos(latitude)
    quad_weight = cosine_lat * (math.pi / lat_count)
    order_m = jnp.full((1, lat_count), order, jnp.int32).astype(jnp.float32)
    counter = lax.broadcasted_iota(jnp.int32, (1, lat_count), 1).astype(jnp.float32) + 1.0
    increments = 0.5 * jnp.log((2.0 * counter + 1.0) / (2.0 * counter))
    summed = jnp.sum(jnp.where(counter <= order_m, increments, 0.0), axis=1, keepdims=True)
    current = jnp.exp(0.5 * math.log(0.5) + summed + order_m * jnp.log(cosine_lat))
    previous = jnp.zeros_like(current)
    ratio_prev = jnp.ones_like(current)
    table[0:1, :] = current
    for offset in range(1, wave_count):
        degree = order_m + float(offset)
        ratio = jnp.sqrt((4.0 * degree * degree - 1.0) / (degree * degree - order_m * order_m))
        following = ratio * (sine_lat * current - previous / ratio_prev)
        previous, current, ratio_prev = current, following, ratio
        table[offset : offset + 1, :] = current
    degree = (
        lax.broadcasted_iota(jnp.int32, (wave_count, lat_count), 0) + order
    ).astype(jnp.float32)
    kept = degree <= wave_count - 1
    poly = jnp.where(kept, table[...], 0.0)
    damping = jnp.where(
        kept, 1.0 / (1.0 + degree * (degree + 1.0) / (wave_count * (wave_count - 1.0))), 0.0
    )
    scale = jnp.where(order_m > 0.0, 2.0 / NLON, 1.0 / NLON)
    weighted = poly * quad_weight
    poly = poly * scale
    forward_ref[...] = jnp.dot(
        poly.T, damping * weighted, precision=highest, preferred_element_type=jnp.float32
    )
    backward_ref[...] = jnp.dot(
        weighted.T, damping * poly, precision=highest, preferred_element_type=jnp.float32
    )


def vmem(count):
    return [pl.BlockSpec(memory_space=pltpu.VMEM)] * count


def nbytes(shape, dtype):
    return math.prod(shape) * jnp.dtype(dtype).itemsize


def call(kernel, shapes, *operands, name, scratch=(), fetched=0, spare=4):
    here = len(operands) - fetched
    held = [(operand.shape, operand.dtype) for operand in operands[:here]]
    held += list(shapes) + list(scratch)
    operands = operands[:here] + tuple(
        pltpu.with_memory_space_constraint(operand, pltpu.HBM) for operand in operands[here:]
    )
    return pl.pallas_call(
        kernel,
        out_shape=tuple(jax.ShapeDtypeStruct(shape, dtype) for shape, dtype in shapes),
        in_specs=vmem(here) + [pl.BlockSpec(memory_space=pltpu.HBM)] * fetched,
        out_specs=tuple(vmem(len(shapes))),
        scratch_shapes=[pltpu.VMEM(shape, dtype) for shape, dtype in scratch]
        + [pltpu.SemaphoreType.DMA((fetched + 3,))] * bool(fetched),
        name=name,
        compiler_params=pltpu.CompilerParams(
            vmem_limit_bytes=sum(nbytes(*each) for each in held) + spare * 1024 * 1024
        ),
    )(*operands)


def mm(left, right):
    return jnp.dot(left, right, preferred_element_type=jnp.float32)


def mm_nt(left, right):
    return lax.dot_general(
        left, right, (((1,), (1,)), ((), ())), preferred_element_type=jnp.float32
    )


def mm_tn(left, right):
    return lax.dot_general(
        left, right, (((0,), (0,)), ((), ())), preferred_element_type=jnp.float32
    )


def split(value):
    high = value.astype(jnp.bfloat16)
    return high, (value - high.astype(jnp.float32)).astype(jnp.bfloat16)


def mm_fine(left, right):
    left_high, left_low = split(left)
    right_high, right_low = split(right)
    return mm(left_high, right_high) + (mm(left_high, right_low) + mm(left_low, right_high))


def silu_pair(value):
    gate = jax.nn.sigmoid(value)
    return value * gate, gate * (1.0 + value * (1.0 - gate))


def wave_table(transposed):
    shape = (NLON, 2 * MW) if transposed else (2 * MW, NLON)
    lon = lax.broadcasted_iota(jnp.int32, shape, 0 if transposed else 1)
    row = lax.broadcasted_iota(jnp.int32, shape, 1 if transposed else 0)
    wave = jnp.where(row >= MW, row - MW, row)
    angle = ((lon * wave) & (NLON - 1)).astype(jnp.float32) * (2.0 * math.pi / NLON)
    return jnp.where(row >= MW, -jnp.sin(angle), jnp.cos(angle))


def store_waves(table, fields, out_ref):
    waves = mm_fine(table, jnp.concatenate(fields, axis=1))
    feat = fields[0].shape[1]
    for i in range(len(fields)):
        for p in range(2):
            out_ref[:, 2 * i + p, :] = waves[p * MW : (p + 1) * MW, i * feat : (i + 1) * feat]


def load_fields(table_t, waves_ref):
    columns = [
        jnp.concatenate([waves_ref[:, 2 * i, :], waves_ref[:, 2 * i + 1, :]], axis=0)
        for i in range(4)
    ]
    feat = columns[0].shape[1]
    grid = mm_fine(table_t, jnp.concatenate(columns, axis=1))
    return [grid[:, i * feat : (i + 1) * feat] for i in range(4)]


def physics(rows, w_first, w_middle, h1_ref, s1_ref, h2_ref, s2_ref, at):
    size = rows.shape[0]
    half = h1_ref.shape[2]
    value, slope = silu_pair(mm(rows, w_first[...]))
    hidden = value.astype(jnp.bfloat16)
    h1_ref[0, at : at + size, :] = hidden[:, :half]
    h1_ref[1, at : at + size, :] = hidden[:, half:]
    s1_ref[at : at + size, :] = slope
    value, slope = silu_pair(mm(hidden, w_middle[...]))
    h2_ref[at : at + size, :] = value.astype(jnp.bfloat16)
    s2_ref[at : at + size, :] = slope


def first_kernel(
    state_hbm, cotangent_hbm, w_first_hbm, w_middle_hbm, w_last_hbm,
    waves, x, w_first, w_middle, w_last, table, table_t, forward_op, backward_op, h1, s1, h2, s2,
    state, cotangent, poly, sem,
):
    piece = w_middle.shape[0] // 4
    parts = [pl.ds(i * piece, piece) for i in range(4)]
    pairs = [(w_middle_hbm.at[part], w_middle.at[part]) for part in parts] + [
        (state_hbm, state),
        (w_first_hbm, w_first),
        (w_last_hbm, w_last),
        (cotangent_hbm, cotangent),
    ]
    copies = [
        pltpu.make_async_copy(start, end, sem.at[i]) for i, (start, end) in enumerate(pairs)
    ]
    for copy in copies:
        copy.start()
    table[...] = wave_table(False)
    table_t[...] = wave_table(True)
    legendre(forward_op.shape[0], MW, lax.axis_index(LAT), forward_op, backward_op, poly)
    for copy in copies:
        copy.wait()
    field = jnp.concatenate([state[0, 0], state[0, 1]], axis=0)
    x[...] = field.astype(jnp.bfloat16)
    physics(x[...], w_first, w_middle, h1, s1, h2, s2, 0)
    moved = field + tend_weight * mm(h2[...], w_last[...])
    store_waves(
        table[...], [moved[:NLON], moved[NLON:], cotangent[0, 0], cotangent[0, 1]], waves
    )


def middle_kernel(
    waves_in, table, table_t, w_first, w_middle, w_last,
    waves, x, h1, h2, ga1, ga2, gt, s1, s2,
):
    fields = load_fields(table_t[...], waves_in)
    field = jnp.concatenate(fields[:2], axis=0)
    pulled = jnp.concatenate(fields[2:], axis=0)
    x[...] = field.astype(jnp.bfloat16)
    gt[...] = (tend_weight * pulled).astype(jnp.bfloat16)
    physics(x[...], w_first, w_middle, h1, s1, h2, s2, 0)
    moved = field + tend_weight * mm(h2[...], w_last[...])
    ga2[...] = (mm_nt(gt[...], w_last[...]) * s2[...]).astype(jnp.bfloat16)
    ga1[...] = (mm_nt(ga2[...], w_middle[...]) * s1[...]).astype(jnp.bfloat16)
    grad = pulled + mm_nt(ga1[...], w_first[...])
    store_waves(table[...], [moved[:NLON], moved[NLON:], grad[:NLON], grad[NLON:]], waves)


def last_kernel(
    waves_in, table_t, h1_0, s2, h1_1, ga2_1, w_last,
    final, send, ga2, gt,
):
    fields = load_fields(table_t[...], waves_in)
    for j in range(2):
        final[j] = fields[j]
        gt[j * NLON : (j + 1) * NLON, :] = (tend_weight * fields[2 + j]).astype(jnp.bfloat16)
    ga2[...] = (mm_nt(gt[...], w_last[...]) * s2[...]).astype(jnp.bfloat16)
    which = 1 - lax.axis_index("c")
    send[...] = mm_tn(h1_0[which], ga2[...]) + mm_tn(h1_1[which], ga2_1[...])


def thin_kernel(
    x_0, h2_0, s1, ga2, gt_0, w_middle, x_1, h2_1, ga1_1, gt_1,
    keep, send, ga1, first, last,
):
    ga1[...] = (mm_nt(ga2[...], w_middle[...]) * s1[...]).astype(jnp.bfloat16)
    first[...] = mm_tn(x_0[...], ga1[...]) + mm_tn(x_1[...], ga1_1[...])
    last[...] = mm_tn(h2_0[...], gt_0[...]) + mm_tn(h2_1[...], gt_1[...])
    core = lax.axis_index("c")
    part, blocks = keep.shape[0] // 2, 8
    half = part * blocks
    for out, which in ((send, 1 - core), (keep, core)):
        out[0:part, :] = first[pl.ds(pl.multiple_of(which * part, part), part), :]
        for b in range(blocks):
            at = pl.multiple_of(which * half + b * part, part)
            out[part : 2 * part, b * 128 : (b + 1) * 128] = last[pl.ds(at, part), :]


def keep_kernel(h1_0, ga2_0, h1_1, ga2_1, keep):
    core = lax.axis_index("c")
    keep[...] = mm_tn(h1_0[core], ga2_0[...]) + mm_tn(h1_1[core], ga2_1[...])


def latitudes_kernel(owned, forward_op, backward_op, back):
    for i, operator in ((0, forward_op), (1, backward_op)):
        parts = [
            jnp.concatenate([owned[:, 4 * i + p, :], owned[:, 4 * i + 2 + p, :]], axis=0)
            for p in range(2)
        ]
        found = mm_fine(operator[...], jnp.concatenate(parts, axis=1))
        bands = owned.shape[0]
        feat = owned.shape[2]
        for j in range(2):
            for p in range(2):
                back[:, 4 * i + 2 * j + p, :] = found[
                    j * bands : (j + 1) * bands, p * feat : (p + 1) * feat
                ]


def sum_wide_kernel(parts, out):
    total = parts[0]
    for i in range(1, parts.shape[0]):
        total = total + parts[i]
    size = out.shape[1]
    for r in range(2):
        for b in range(8):
            out[r * 8 + b] = total[r * size : (r + 1) * size, b * 128 : (b + 1) * 128]


def sum_deep_kernel(parts, out):
    total = parts[0]
    for i in range(1, parts.shape[0]):
        total = total + parts[i]
    for i in range(out.shape[0]):
        out[i] = total


def spread_kernel(parts, out):
    size = parts.shape[1]
    for r in range(2):
        for b in range(8):
            piece = parts[r * 8 + b]
            for i in range(out.shape[0]):
                out[i, r * size : (r + 1) * size, b * 128 : (b + 1) * 128] = piece


def add_kernel(left, left_thin, right, right_thin, out):
    half = left.shape[0]
    out[0:half, :] = left[...] + right[...]
    out[half:, :] = left_thin[...] + right_thin[...]


def place(other, source, outs, sem):
    first, middle, last = outs
    core = lax.axis_index("c")
    which = 1 - core if other else core
    half = middle.shape[0] // 2
    part, blocks = half // 8, 8
    copies = [
        (source.at[pl.ds(0, half)], middle.at[pl.ds(pl.multiple_of(which * half, half), half)]),
        (
            source.at[pl.ds(half, part)],
            first.at[pl.ds(pl.multiple_of(which * part, part), part)],
        ),
    ]
    for b in range(blocks):
        at = pl.multiple_of(which * half + b * part, part)
        copies.append(
            (
                source.at[pl.ds(half + part, part), pl.ds(b * 128, 128)],
                last.at[pl.ds(at, part)],
            )
        )
    started = [
        pltpu.make_async_copy(start, end, sem.at[i]) for i, (start, end) in enumerate(copies)
    ]
    for copy in started:
        copy.start()
    for copy in started:
        copy.wait()


def own_kernel(source, first, middle, last, sem):
    place(False, source, (first, middle, last), sem)


def other_kernel(source, _first, _middle, _last, first, middle, last, sem):
    place(True, source, (first, middle, last), sem)


def unpack(own, other, hidden, features):
    outs = [
        jax.ShapeDtypeStruct(shape, jnp.float32)
        for shape in ((features, hidden), (hidden, hidden), (hidden, features))
    ]
    hbm = pl.BlockSpec(memory_space=pltpu.HBM)
    settings = dict(
        out_shape=tuple(outs),
        out_specs=(hbm,) * 3,
        scratch_shapes=[pltpu.SemaphoreType.DMA((10,))],
        compiler_params=pltpu.CompilerParams(vmem_limit_bytes=4 * 1024 * 1024),
    )
    grads = pl.pallas_call(own_kernel, in_specs=vmem(1), name="own", **settings)(own)
    return pl.pallas_call(
        other_kernel,
        in_specs=vmem(1) + [hbm] * 3,
        input_output_aliases={1: 0, 2: 1, 3: 2},
        name="other",
        **settings,
    )(other, *grads)


def body(state, cotangent, w_first, w_middle, w_last):
    _, lat_rows, lon_count, features = state.shape
    hidden = w_first.shape[1]
    rows = lat_rows * lon_count
    bands = lax.axis_size("xl") * lax.axis_size("z") * lax.axis_size("y")
    f32, bf16 = jnp.float32, jnp.bfloat16
    waves_of = ((MW, 8, features), f32)
    halves = ((2, rows, hidden // 2), bf16)
    wide16, wide32 = ((rows, hidden), bf16), ((rows, hidden), f32)
    thin16 = ((rows, features), bf16)
    part = ((lat_rows, lon_count, features), f32)
    square = ((lat_rows * bands,) * 2, f32)

    def cross(waves):
        owned = lax.all_to_all(waves, LAT, 0, 0, tiled=True)
        (back,) = call(
            latitudes_kernel, [waves_of], owned, forward_op, backward_op, name="latitudes"
        )
        return lax.all_to_all(back, LAT, 0, 0, tiled=True)

    (
        waves, x_0, w_first, w_middle, w_last, table, table_t, forward_op, backward_op,
        h1_0, s1_0, h2_0, s2_0,
    ) = call(
        first_kernel,
        [
            waves_of, thin16,
            (w_first.shape, bf16), (w_middle.shape, bf16), (w_last.shape, bf16),
            ((2 * MW, NLON), f32), ((NLON, 2 * MW), f32), square, square,
            halves, wide32, wide16, wide32,
        ],
        state, cotangent, w_first, w_middle, w_last,
        name="first",
        fetched=5,
        scratch=[(state.shape, f32), (state.shape, f32), ((MW, lat_rows * bands), f32)],
    )
    waves = cross(waves)
    waves, x_1, h1_1, h2_1, ga1_1, ga2_1, gt_1 = call(
        middle_kernel,
        [waves_of, thin16, halves, wide16, wide16, wide16, thin16],
        waves, table, table_t, w_first, w_middle, w_last,
        name="middle",
        scratch=[wide32] * 2,
    )
    waves = cross(waves)
    packed = ((hidden // 2 + features, hidden), f32)
    half32, thin32 = ((hidden // 2, hidden), f32), ((features, hidden), f32)
    final, send, ga2_0, gt_0 = call(
        last_kernel,
        [part, half32, wide16, thin16],
        waves, table_t, h1_0, s2_0, h1_1, ga2_1, w_last,
        name="last",
    )
    received = lax.ppermute(send, "c", SWAP)
    keep_thin, send_thin = call(
        thin_kernel,
        [thin32, thin32],
        x_0, h2_0, s1_0, ga2_0, gt_0, w_middle, x_1, h2_1, ga1_1, gt_1,
        name="thin",
        scratch=[wide16, thin32, ((hidden, features), f32)],
    )
    received_thin = lax.ppermute(send_thin, "c", SWAP)
    (keep,) = call(
        keep_kernel, [half32], h1_0, ga2_0, h1_1, ga2_1, name="keep"
    )
    (held,) = call(
        add_kernel, [packed], keep, keep_thin, received, received_thin, name="add"
    )
    wide, deep = len(WIDE[0]), len(DEEP[0])
    piece = packed[0][0] // wide
    held = exchange(held.reshape(wide, piece, hidden), WIDE)
    parts = ((deep, piece // 2, hidden // 8), f32)
    (held,) = call(sum_wide_kernel, [parts], held, name="sum_wide")
    held = exchange(held, DEEP)
    (held,) = call(sum_deep_kernel, [parts], held, name="sum_deep")
    held = exchange(held, DEEP)
    (held,) = call(spread_kernel, [((wide, piece, hidden), f32)], held, name="spread")
    held = exchange(held, WIDE).reshape(packed[0])
    other = lax.ppermute(held, "c", SWAP)
    first, middle, last = unpack(held, other, hidden, features)
    return final[None], first, middle, last


def solution(mesh):
    fine = Mesh(mesh.devices.reshape(tuple(size for _, size in FINE)), ALL)
    grid = P(("xh", "c"), BAND, None, None)
    return jax.shard_map(
        body,
        mesh=fine,
        in_specs=(grid, grid, P(), P(), P()),
        out_specs=(grid, P(), P(), P()),
        check_vma=False,
    )
```
